256 devices in a mesh: frow: 16 (over x_lo, y, core), fcol: 16 (over z, x_hi).
Axes of the slice: x: 4 (x_hi: 2, x_lo: 2; x = x_hi * 2 + x_lo), y: 4, z: 8, core: 2. Of those that a mesh axis runs over, the one named last changes fastest.
Arguments:
- facets: float32 [2, 16384, 16384], P(None, 'frow', 'fcol'), may hold values from -6 to 6
- facet_row_offset: int32 [16], P('frow'), may hold values from 0 to 16383
- facet_col_offset: int32 [16], P('fcol'), may hold values from 0 to 16383
- strip_offset: int32 [4], replicated, may hold values from 0 to 16383
- subgrid_strip: int32 [48], replicated, may hold values from 0 to 3
- subgrid_column: int32 [48], replicated, may hold values from 0 to 16383
- subgrid_slot: int32 [48], replicated, may hold values from 0 to 47, each once
Outputs:
- subgrids: float32 [48, 2, 128, 128], P('frow', None, 'fcol')
The draws below stay inside these ranges and needn't reach their ends.
Inputs may be any that keep to these rules, and one draw needn't show every extreme that they name: `subgrid_slot`: every slot from 0 to 47 is named by exactly one subgrid.
All inputs are finite; a program needn't handle non-finite values.
Results may differ from the reference program's by a relative error of at most 0.0003.
Values sent between devices are 32-bit elements; how exact they have to be, the bound alone decides.
A program may use at most 64 MiB of HBM per device.

```python
import math
import jax
import jax.numpy as jnp
from jax import lax

F = 1024
M = 128
STRIPS = 4
NR = 16384
NC = 16384
SUBGRIDS = 48
N_FROW = 16
N_FCOL = 16


def plant(values, stream_key, smallest, largest):
    longest = values.shape.index(max(values.shape))
    spots = []
    for shift in (0, 1):
        where = [jax.random.randint(jax.random.fold_in(stream_key, axis), (), 0, length) for axis, length in enumerate(values.shape)]
        where[longest] = (where[longest] + shift) % values.shape[longest]
        spots.append(tuple(where))
    return values.at[spots[0]].set(smallest).at[spots[1]].set(largest)


def level_of(key, shape, pieces, low, high):
    def one(dim, parts):
        draws = jax.random.uniform(jax.random.fold_in(jax.random.fold_in(key, 6), dim), (parts,), jnp.float32, low / len(pieces), high / len(pieces))
        return jnp.repeat(jnp.exp(draws), shape[dim] // parts).reshape((-1,) + (1,) * (len(shape) - dim - 1))

    level = one(*pieces[0])
    for cut in pieces[1:]:
        level = level * one(*cut)
    return level


def scatter_about(own_key, extent, scale, most, split=(), kind=jnp.bfloat16):
    gain = level_of(own_key, extent, split, -0.22, 0.18) if split else 1.0
    array = jax.random.normal(own_key, extent, jnp.float32) * scale * gain
    return jnp.minimum(jnp.maximum(array, -most), most).astype(kind)


def setup_inputs(seed: int = 0) -> dict:
    seeds = jax.random.split(jax.random.key(seed), 8)
    return {
        "facets": scatter_about(seeds[0], (2, NR, NC), 1.0, 6.0, ((1, 16), (2, 16)), jnp.float32),
        "facet_row_offset": plant(jax.random.randint(seeds[1], (N_FROW,), 0, NR), jax.random.fold_in(seeds[1], 1), 0, NR - 1).astype(jnp.int32),
        "facet_col_offset": plant(jax.random.randint(seeds[2], (N_FCOL,), 0, NC), jax.random.fold_in(seeds[2], 1), 0, NC - 1).astype(jnp.int32),
        "strip_offset": plant(jax.random.randint(seeds[3], (STRIPS,), 0, NR), jax.random.fold_in(seeds[3], 1), 0, NR - 1).astype(jnp.int32),
        "subgrid_strip": plant(jax.random.randint(seeds[4], (SUBGRIDS,), 0, STRIPS), jax.random.fold_in(seeds[4], 1), 0, STRIPS - 1).astype(jnp.int32),
        "subgrid_column": plant(jax.random.randint(seeds[5], (SUBGRIDS,), 0, NC), jax.random.fold_in(seeds[5], 1), 0, NC - 1).astype(jnp.int32),
        "subgrid_slot": jax.random.permutation(seeds[6], SUBGRIDS).astype(jnp.int32),
    }


HIGHEST_PRECISION = lax.Precision.HIGHEST

def window(width):
    return jnp.sin(math.pi * (jnp.arange(width, dtype=jnp.int32).astype(jnp.float32) + 0.5) / width)

def phase_table(pixels, frequencies, weights, modulus):
    products = frequencies[..., :, None] * pixels % modulus
    angles = products.astype(jnp.float32) * (2.0 * math.pi / modulus)
    norm_scale = 1.0 / math.sqrt(modulus)
    real_table = weights * jnp.cos(angles) * norm_scale
    imag_table = -(weights * jnp.sin(angles)) * norm_scale
    return (real_table, imag_table)

def reference(facets, facet_row_offset, facet_col_offset, strip_offset, subgrid_strip, subgrid_column, subgrid_slot):
    pixel_steps = jnp.arange(F, dtype=jnp.int32)
    spectrum = jnp.arange(M, dtype=jnp.int32)
    row_pixels = ((facet_row_offset[:, None] + pixel_steps[None, :]) % NR).reshape(NR)
    col_pixels = ((facet_col_offset[:, None] + pixel_steps[None, :]) % NC).reshape(NC)
    row_weights = jnp.tile(window(F), N_FROW)
    col_weights = jnp.tile(window(F), N_FCOL)
    frequencies = (strip_offset[:, None] + spectrum[None, :]) % NR
    row_real, row_imag = phase_table(row_pixels, frequencies, row_weights, NR)
    stacked = jnp.concatenate([row_real, row_imag], 0).reshape(2 * STRIPS * M, NR)
    upper_rows = jnp.dot(stacked, facets[0], precision=HIGHEST_PRECISION, preferred_element_type=jnp.float32)
    bottom = jnp.dot(stacked, facets[1], precision=HIGHEST_PRECISION, preferred_element_type=jnp.float32)
    half_rows = STRIPS * M
    strip_real = upper_rows[:half_rows] - bottom[half_rows:]
    strip_imag = bottom[:half_rows] + upper_rows[half_rows:]
    strips = jnp.stack([strip_real.reshape(STRIPS, M, NC), strip_imag.reshape(STRIPS, M, NC)], 1)

    def one_subgrid(subgrid_index):
        chosen = strips[subgrid_strip[subgrid_index]].reshape(2 * M, NC)
        col_frequencies = (subgrid_column[subgrid_index] + spectrum) % NC
        col_real, col_imag = phase_table(col_pixels, col_frequencies, col_weights, NC)
        columns_table = jnp.concatenate([col_real, col_imag], 0)
        product = jnp.einsum('qf,pf->qp', chosen, columns_table, precision=HIGHEST_PRECISION, preferred_element_type=jnp.float32)
        real_sum = product[:M, :M] - product[M:, M:]
        imag_sum = product[:M, M:] + product[M:, :M]
        return jnp.stack([real_sum, imag_sum])
    grids = lax.map(one_subgrid, jnp.arange(SUBGRIDS, dtype=jnp.int32))
    return jnp.zeros_like(grids).at[subgrid_slot].set(grids)
```

```python
import math

import jax
import jax.numpy as jnp
from jax import lax
from jax.experimental import pallas as pl
from jax.experimental.pallas import tpu as pltpu
from jax.sharding import PartitionSpec as P

F = 1024
M = 128
N = 16384
MASK = N - 1
SLOTS = 48
CW = 256
NT = F // CW
f32 = jnp.float32
bf16 = jnp.bfloat16
MESH = pl.DeviceIdType.MESH

FLIP = (8, 2, 6)
ORDERS = ((0, 1, 2), (1, 2, 0), (2, 0, 1))


def groups_of(u):
    cuts = ((0, 2), (2, 1), (3, 1))
    return [(ORDERS[(u + g) % 3], c0, n) for g, (c0, n) in enumerate(cuts)]


def iota(shape, dim):
    return lax.broadcasted_iota(jnp.int32, shape, dim)


def cos_sin(m):
    q = (m + N // 8) >> 12
    x = (m - (q << 12)).astype(f32) * (2.0 * math.pi / N)
    x2 = x * x
    s = x * (1.0 + x2 * (-1.0 / 6 + x2 * (1.0 / 120 + x2 * (-1.0 / 5040 + x2 * (1.0 / 362880)))))
    c = 1.0 + x2 * (-0.5 + x2 * (1.0 / 24 + x2 * (-1.0 / 720 + x2 * (1.0 / 40320))))
    swap = (q & 1) == 1
    cos = jnp.where(swap, s, c)
    sin = jnp.where(swap, c, s)
    cos = jnp.where(((q + 1) & 2) == 2, -cos, cos)
    sin = jnp.where((q & 2) == 2, -sin, sin)
    return cos, sin


def window(j):
    x = (jnp.minimum(j, F - 1 - j).astype(f32) + 0.5) * (math.pi / F)
    x2 = x * x
    poly = 1.0 / 6227020800
    for k in (-39916800, 362880, -5040, 120, -6, 1):
        poly = poly * x2 + 1.0 / k
    return poly * x * (1.0 / math.sqrt(N))


def split(x):
    hi = x.astype(bf16)
    return hi, (x - hi.astype(f32)).astype(bf16)


def dot3(ah, al, bh, bl):
    def d(a, b):
        return jnp.dot(a, b, preferred_element_type=f32)

    return d(ah, bh) + d(ah, bl) + d(al, bh)


def kernel(
    x_hbm, roff, coff, soff, strip_of, col_of, out_ref,
    xf, xh, xl, th, tl, ut, vt, s, rd, r0, r1, r2,
    fb, ph, eh, el, ah, al, gacc, g, ra, pb, rb,
    x_sem, d_ssem, d_rsem, e_ssem, e_rsem, a_ssem, a_rsem, b_ssem, b_rsem,
):
    i = lax.axis_index("frow")
    j = lax.axis_index("fcol")
    core = i & 1
    y = (i >> 1) & 3
    xlo = i >> 3
    z = j >> 1
    xhi = j & 1
    own = (xlo, (y ^ (y >> 1)) & 1, y >> 1)
    kz = own[0] * 4 + own[1] * 2 + own[2]
    recv_bufs = (r0, r1, r2)

    def x_copy(t):
        return pltpu.make_async_copy(
            x_hbm.at[:, :, pl.ds(t * CW, CW)], xf.at[t], x_sem.at[t]
        )

    for t in range(NT):
        x_copy(t).start()

    barrier = pltpu.get_barrier_semaphore()

    def hello(fr, fc):
        pl.semaphore_signal(barrier, inc=1, device_id=(fr, fc), device_id_type=MESH)

    for flip in (1, *FLIP):
        hello(i ^ flip, j)

    @pl.loop(0, 8)
    def _(p):
        for xs in range(2):
            src_i = p * 2 + xhi
            src_j = z * 2 + xs

            @pl.when(jnp.logical_or(src_i != i, src_j != j))
            def _():
                hello(src_i, src_j)

        @pl.when(p != z)
        def _():
            hello(i, p * 2 + xhi)

    def wait_barrier():
        pl.semaphore_wait(barrier, 27 - (1 - (core ^ xhi)))

    def gen_u():
        row = iota((64, 1), 0)
        c = row & 3
        kb = row >> 2
        block = ((kb & 7) << 1) | (kb >> 3)
        f = jnp.where(c == 0, soff[0], jnp.where(c == 1, soff[1], jnp.where(c == 2, soff[2], soff[3])))
        f = f + 8 * block
        for b in range(4):
            p = roff[0] + b * 256 + iota((1, 256), 1)
            cos, sin = cos_sin((f * p) & MASK)
            ut[0, :, b * 256 : (b + 1) * 256] = cos
            ut[1, :, b * 256 : (b + 1) * 256] = sin

    def gen_t(h):
        r = iota((8, 1), 0)
        jj = iota((1, F), 1)
        m = ((r & 3) + 4 * h) * (roff[0] + jj) + (r >> 2) * (N // 4)
        cos, sin = cos_sin(m & MASK)
        w = window(jj)
        vt[0] = w * cos
        vt[1] = w * sin

        for b in range(4):
            cols = slice(b * 256, (b + 1) * 256)
            right = slice(F + b * 256, F + (b + 1) * 256)
            vr = vt[0, :, cols]
            vi = vt[1, :, cols]
            for kb in range(16):
                left_t, right_t = [], []
                for c in range(4):
                    q = kb * 4 + c
                    ur = ut[0, q : q + 1, cols]
                    ui = ut[1, q : q + 1, cols]
                    left_t.append(ur * vr - ui * vi)
                    right_t.append(ui * vr + ur * vi)
                hi, lo = split(jnp.concatenate(left_t, 0))
                th[h, kb, :, cols] = hi
                tl[h, kb, :, cols] = lo
                hi, lo = split(jnp.concatenate(right_t, 0))
                th[h, kb, :, right] = hi
                tl[h, kb, :, right] = lo

    def split_x(t):
        @pl.loop(0, 8)
        def _(b):
            rows = pl.ds(pl.multiple_of(b * 128, 128), 128)
            for part in range(2):
                hi, lo = split(xf[t, part, rows, :])
                dst = pl.ds(pl.multiple_of(part * F + b * 128, 128), 128)
                xh[t, dst, :] = hi
                xl[t, dst, :] = lo

    def gen_cols():
        for b in range(4):
            jj = b * 256 + iota((1, 256), 1)
            cos, sin = cos_sin((col_of[...] * (coff[0] + jj)) & MASK)
            w = window(jj)
            ph[0, :, b * 256 : (b + 1) * 256] = w * cos
            ph[1, :, b * 256 : (b + 1) * 256] = -(w * sin)

        @pl.loop(0, 32)
        def _(b):
            n = b * 32 + iota((32, 1), 0)
            m = (iota((1, M), 1) * (coff[0] + n)) & MASK
            cos, sin = cos_sin(m)
            hi, lo = split(jnp.concatenate([cos, -sin], 1))
            rows = pl.ds(pl.multiple_of(b * 32, 32), 32)
            eh[rows, :] = hi
            el[rows, :] = lo

    def matmul(u):
        h, t = divmod(u, NT)
        out = dot3(
            th[h].reshape(512, 2 * F), tl[h].reshape(512, 2 * F), xh[t], xl[t]
        )
        s[u] = out.reshape(2, 2, 2, 2, 4, 8, CW)

    def d2d(u):
        return pltpu.make_async_remote_copy(
            src_ref=s.at[u, 1 - core],
            dst_ref=rd.at[u],
            send_sem=d_ssem.at[u],
            recv_sem=d_rsem.at[u],
            device_id=(i ^ 1, j),
            device_id_type=MESH,
        )

    def region(order, k, c0, n, other):
        sel = [slice(None)] * 3
        for d in order[:k]:
            sel[d] = own[d]
        sel[order[k]] = 1 - own[order[k]] if other else own[order[k]]
        return (*sel, slice(c0, c0 + n))

    def exchange(u, k, gi):
        order, c0, n = groups_of(u)[gi]
        return pltpu.make_async_remote_copy(
            src_ref=s.at[(u, core, *region(order, k, c0, n, True))],
            dst_ref=recv_bufs[k].at[(u, *[slice(None)] * (2 - k), slice(c0, c0 + n))],
            send_sem=e_ssem.at[u, k, gi],
            recv_sem=e_rsem.at[u, k, gi],
            device_id=(i ^ FLIP[order[k]], j),
            device_id_type=MESH,
        )

    def finish_d2d(u):
        d2d(u).wait_recv()
        s[u, core] += rd[u]
        for gi in range(3):
            exchange(u, 0, gi).start()

    def finish_exchange(u, k):
        for gi, (order, c0, n) in enumerate(groups_of(u)):
            exchange(u, k, gi).wait_recv()
            at = (u, core, *region(order, k, c0, n, False))
            s[at] += recv_bufs[k][(u, *[slice(None)] * (2 - k), slice(c0, c0 + n))]
            if k < 2:
                exchange(u, k + 1, gi).start()

    sign = jnp.where(iota((8, 1), 0) < 4, -1.0, 1.0).astype(f32)

    def columns(u):
        h, t = divmod(u, NT)
        cols = slice(t * CW, (t + 1) * CW)
        for c in range(4):
            tile = s[u, core, own[0], own[1], own[2], c]
            fb[0, c] = tile
            fb[1, c] = jnp.concatenate([tile[4:], tile[:4]], 0) * sign
        for q0 in range(0, SLOTS, 4):
            tiles = []
            for q in range(q0, q0 + 4):
                st = strip_of[q]
                tiles.append(fb[0, st] * ph[0, q : q + 1, cols] + fb[1, st] * ph[1, q : q + 1, cols])
            hi, lo = split(jnp.concatenate(tiles, 0))
            ah[q0 * 8 : (q0 + 4) * 8, :] = hi
            al[q0 * 8 : (q0 + 4) * 8, :] = lo
        prod = dot3(ah[...], al[...], eh[cols, :], el[cols, :])
        if t == 0:
            gacc[...] = prod
        elif t < NT - 1:
            gacc[...] += prod
        else:
            total = (gacc[...] + prod).reshape(SLOTS, 8, 2 * M)
            cross = total[:, :, M:]
            cross = jnp.concatenate([cross[:, 4:], cross[:, :4]], 1)
            g[h] = total[:, :, :M] + cross * sign

    def a_copy(h, a):
        return pltpu.make_async_remote_copy(
            src_ref=g.at[h, pl.ds(3 * a, 3)],
            dst_ref=ra.at[h, xhi, kz],
            send_sem=a_ssem.at[h, a],
            recv_sem=a_rsem.at[h, xhi, kz],
            device_id=(a, z * 2 + core),
            device_id_type=MESH,
        )

    def a_remote(a):
        return jnp.logical_or(a != i, core != xhi)

    def start_a(h):
        @pl.loop(0, 16)
        def _(n):
            a = (n + i) & 15

            @pl.when(a_remote(a))
            def _():
                a_copy(h, a).start()

        @pl.when(core == xhi)
        def _():
            ra[h, xhi, kz] = g[h, pl.ds(3 * i, 3)]

    def b_copy(h, k):
        return pltpu.make_async_remote_copy(
            src_ref=pb.at[h, k],
            dst_ref=rb.at[h, z],
            send_sem=b_ssem.at[h, k],
            recv_sem=b_rsem.at[h, z],
            device_id=(i, k * 2 + xhi),
            device_id_type=MESH,
        )

    def a_arrival(h, xs, k):
        return pltpu.make_async_remote_copy(
            src_ref=g.at[h, pl.ds(0, 3)],
            dst_ref=ra.at[h, xs, k],
            send_sem=a_ssem.at[h, 0],
            recv_sem=a_rsem.at[h, xs, k],
            device_id=(i, j),
            device_id_type=MESH,
        )

    def b_arrival(h, zs):
        return pltpu.make_async_remote_copy(
            src_ref=pb.at[h, 0],
            dst_ref=rb.at[h, zs],
            send_sem=b_ssem.at[h, 0],
            recv_sem=b_rsem.at[h, zs],
            device_id=(i, j),
            device_id_type=MESH,
        )

    def finish_a(h):
        @pl.loop(0, 8)
        def _(n):
            k = (n + z + 1) & 7
            for xs in range(2):
                mine = jnp.logical_and(core == xhi, jnp.logical_and(xhi == xs, k == kz))

                @pl.when(jnp.logical_not(mine))
                def _():
                    a_arrival(h, xs, k).wait_recv()

            pb[h, k] = ra[h, 0, k] + ra[h, 1, k]

            @pl.when(k != z)
            def _():
                b_copy(h, k).start()

    def finish_b(h):
        rb[h, z] = pb[h, z]

        @pl.loop(0, 8)
        def _(zs):
            @pl.when(zs != z)
            def _():
                b_arrival(h, zs).wait_recv()

        total = rb[h, 0]
        for zs in range(1, 8):
            total = total + rb[h, zs]
        out_ref[:, 0, 4 * h : 4 * h + 4, :] = total[:, :4]
        out_ref[:, 1, 4 * h : 4 * h + 4, :] = total[:, 4:]

    gen_u()
    gen_t(0)
    slots = 2 * NT
    for v in range(slots + 4):
        if v < NT:
            x_copy(v).wait()
            split_x(v)
        if v == 1:
            gen_cols()
        if v == NT:
            gen_t(1)
        if v < slots:
            matmul(v)
            if v == 0:
                wait_barrier()
            d2d(v).start()
        if 0 <= v - 1 < slots:
            finish_d2d(v - 1)
        for k in range(3):
            if 0 <= v - 2 - k < slots:
                finish_exchange(v - 2 - k, k)
        if 0 <= v - 4 < slots:
            columns(v - 4)
            if v - 4 == NT - 1:
                start_a(0)
        if v == slots + 1:
            finish_a(0)
    start_a(1)
    finish_b(0)
    finish_a(1)
    finish_b(1)

    for u in range(slots):
        d2d(u).wait_send()
        for k in range(3):
            for gi in range(3):
                exchange(u, k, gi).wait_send()

    @pl.loop(0, 16)
    def _(a):
        for h in range(2):

            @pl.when(a_remote(a))
            def _():
                a_copy(h, a).wait_send()

    @pl.loop(0, 8)
    def _(k):
        for h in range(2):

            @pl.when(k != z)
            def _():
                b_copy(h, k).wait_send()


def per_device(facets, row_off, col_off, strip_offset, subgrid_strip, subgrid_column, subgrid_slot):
    ids = jnp.arange(SLOTS, dtype=jnp.int32)
    hit = subgrid_slot[None, :] == ids[:, None]
    strip_of = jnp.sum(jnp.where(hit, subgrid_strip[None, :], 0), axis=1)
    col_of = jnp.sum(jnp.where(hit, subgrid_column[None, :], 0), axis=1, keepdims=True)
    smem = pl.BlockSpec(memory_space=pltpu.SMEM)
    vmem = pl.BlockSpec(memory_space=pltpu.VMEM)
    dma = pltpu.SemaphoreType.DMA
    u = 2 * NT
    return pl.pallas_call(
        kernel,
        out_shape=jax.ShapeDtypeStruct((3, 2, 8, M), f32),
        in_specs=[pl.BlockSpec(memory_space=pl.ANY), smem, smem, smem, smem, vmem],
        out_specs=vmem,
        scratch_shapes=[
            pltpu.VMEM((NT, 2, F, CW), f32),
            pltpu.VMEM((NT, 2 * F, CW), bf16),
            pltpu.VMEM((NT, 2 * F, CW), bf16),
            pltpu.VMEM((2, 16, 32, 2 * F), bf16),
            pltpu.VMEM((2, 16, 32, 2 * F), bf16),
            pltpu.VMEM((2, 64, F), f32),
            pltpu.VMEM((2, 8, F), f32),
            pltpu.VMEM((u, 2, 2, 2, 2, 4, 8, CW), f32),
            pltpu.VMEM((u, 2, 2, 2, 4, 8, CW), f32),
            pltpu.VMEM((u, 2, 2, 4, 8, CW), f32),
            pltpu.VMEM((u, 2, 4, 8, CW), f32),
            pltpu.VMEM((u, 4, 8, CW), f32),
            pltpu.VMEM((2, 4, 8, CW), f32),
            pltpu.VMEM((2, SLOTS, F), f32),
            pltpu.VMEM((F, 2 * M), bf16),
            pltpu.VMEM((F, 2 * M), bf16),
            pltpu.VMEM((SLOTS * 8, CW), bf16),
            pltpu.VMEM((SLOTS * 8, CW), bf16),
            pltpu.VMEM((SLOTS * 8, 2 * M), f32),
            pltpu.VMEM((2, SLOTS, 8, M), f32),
            pltpu.VMEM((2, 2, 8, 3, 8, M), f32),
            pltpu.VMEM((2, 8, 3, 8, M), f32),
            pltpu.VMEM((2, 8, 3, 8, M), f32),
            dma((NT,)),
            dma((u,)),
            dma((u,)),
            dma((u, 3, 3)),
            dma((u, 3, 3)),
            dma((2, 16)),
            dma((2, 2, 8)),
            dma((2, 8)),
            dma((2, 8)),
        ],
        compiler_params=pltpu.CompilerParams(
            collective_id=0, has_side_effects=True, vmem_limit_bytes=60 * 1024 * 1024
        ),
        name="facet_to_subgrid",
    )(facets, row_off, col_off, strip_offset, strip_of, col_of)


def solution(mesh):
    placed = (P(None, "frow", "fcol"), P("frow"), P("fcol"), P(), P(), P(), P())
    return jax.shard_map(
        per_device,
        mesh=mesh,
        in_specs=placed,
        out_specs=P("frow", None, "fcol", None),
        check_vma=False,
    )
```

```python
import math

import jax
import jax.numpy as jnp
from jax import lax
from jax.experimental import pallas as pl
from jax.experimental.pallas import tpu as pltpu
from jax.sharding import PartitionSpec as P

F = 1024
M = 128
N = 16384
MASK = N - 1
SLOTS = 48
CW = 256
NT = F // CW
f32 = jnp.float32
bf16 = jnp.bfloat16
MESH = pl.DeviceIdType.MESH

FLIP = (8, 2, 6)
ORDERS = ((0, 1, 2), (1, 2, 0), (2, 0, 1))


def groups_of(u):
    cuts = ((0, 2), (2, 1), (3, 1))
    return [(ORDERS[(u + g) % 3], c0, n) for g, (c0, n) in enumerate(cuts)]


def iota(shape, dim):
    return lax.broadcasted_iota(jnp.int32, shape, dim)


def cos_sin(m):
    q = (m + N // 8) >> 12
    x = (m - (q << 12)).astype(f32) * (2.0 * math.pi / N)
    x2 = x * x
    s = x * (1.0 + x2 * (-1.0 / 6 + x2 * (1.0 / 120 + x2 * (-1.0 / 5040 + x2 * (1.0 / 362880)))))
    c = 1.0 + x2 * (-0.5 + x2 * (1.0 / 24 + x2 * (-1.0 / 720 + x2 * (1.0 / 40320))))
    swap = (q & 1) == 1
    cos = jnp.where(swap, s, c)
    sin = jnp.where(swap, c, s)
    cos = jnp.where(((q + 1) & 2) == 2, -cos, cos)
    sin = jnp.where((q & 2) == 2, -sin, sin)
    return cos, sin


def window(j):
    x = (jnp.minimum(j, F - 1 - j).astype(f32) + 0.5) * (math.pi / F)
    x2 = x * x
    poly = 1.0 / 6227020800
    for k in (-39916800, 362880, -5040, 120, -6, 1):
        poly = poly * x2 + 1.0 / k
    return poly * x * (1.0 / math.sqrt(N))


def split(x):
    hi = x.astype(bf16)
    return hi, (x - hi.astype(f32)).astype(bf16)


def dot3(ah, al, bh, bl):
    def d(a, b):
        return jnp.dot(a, b, preferred_element_type=f32)

    return d(ah, bh) + d(ah, bl) + d(al, bh)


def kernel(
    x_hbm, roff, coff, soff, g_strip, g_column, g_slot, out_ref,
    strip_row, strip_of, col_of, xf, xh, xl, th, tl, ut, vt, s, rd, r0, r1, r2,
    fb, ph, eh, el, ah, al, gacc, g, ra, pb, rb,
    x_sem, st_sem, d_ssem, d_rsem, e_ssem, e_rsem, a_ssem, a_rsem, b_ssem, b_rsem,
):
    i = lax.axis_index("frow")
    j = lax.axis_index("fcol")
    core = i & 1
    y = (i >> 1) & 3
    xlo = i >> 3
    z = j >> 1
    xhi = j & 1
    own = (xlo, (y ^ (y >> 1)) & 1, y >> 1)
    kz = own[0] * 4 + own[1] * 2 + own[2]
    recv_bufs = (r0, r1, r2)

    def x_copy(t):
        return pltpu.make_async_copy(
            x_hbm.at[:, :, pl.ds(t * CW, CW)], xf.at[t], x_sem.at[t]
        )

    for t in range(NT):
        x_copy(t).start()

    barrier = pltpu.get_barrier_semaphore()

    def hello(fr, fc):
        pl.semaphore_signal(barrier, inc=1, device_id=(fr, fc), device_id_type=MESH)

    for flip in (1, *FLIP):
        hello(i ^ flip, j)

    for d in range(1, 16):
        hello((((i >> 1) ^ (d >> 1)) << 1) | xhi, z * 2 + (xhi ^ (d & 1)))

    @pl.when(core != xhi)
    def _():
        hello(i ^ 1, j)

    for d in range(1, 8):
        hello(i, (z ^ d) * 2 + xhi)

    def wait_barrier():
        pl.semaphore_wait(barrier, 27 - (1 - (core ^ xhi)))

    def gen_slots():
        lane = iota((1, 128), 1)
        row = iota((SLOTS, 1), 0)
        strips = jnp.zeros((1, 128), jnp.int32)
        columns_ = jnp.zeros((SLOTS, 1), jnp.int32)
        for n in range(SLOTS):
            strips = jnp.where(lane == g_slot[n], g_strip[n], strips)
            columns_ = jnp.where(row == g_slot[n], g_column[n], columns_)
        strip_row[...] = strips
        col_of[...] = columns_

    def strip_copy():
        return pltpu.make_async_copy(strip_row, strip_of, st_sem.at[0])

    def gen_u():
        row = iota((64, 1), 0)
        c = row & 3
        kb = row >> 2
        block = ((kb & 7) << 1) | (kb >> 3)
        f = jnp.where(c == 0, soff[0], jnp.where(c == 1, soff[1], jnp.where(c == 2, soff[2], soff[3])))
        f = f + 8 * block
        for b in range(4):
            p = roff[0] + b * 256 + iota((1, 256), 1)
            cos, sin = cos_sin((f * p) & MASK)
            ut[0, :, b * 256 : (b + 1) * 256] = cos
            ut[1, :, b * 256 : (b + 1) * 256] = sin

    def gen_t(h):
        r = iota((8, 1), 0)
        jj = iota((1, F), 1)
        m = ((r & 3) + 4 * h) * (roff[0] + jj) + (r >> 2) * (N // 4)
        cos, sin = cos_sin(m & MASK)
        w = window(jj)
        vt[0] = w * cos
        vt[1] = w * sin

        for b in range(4):
            cols = slice(b * 256, (b + 1) * 256)
            right = slice(F + b * 256, F + (b + 1) * 256)
            vr = vt[0, :, cols]
            vi = vt[1, :, cols]
            for kb in range(16):
                left_t, right_t = [], []
                for c in range(4):
                    q = kb * 4 + c
                    ur = ut[0, q : q + 1, cols]
                    ui = ut[1, q : q + 1, cols]
                    left_t.append(ur * vr - ui * vi)
                    right_t.append(ui * vr + ur * vi)
                hi, lo = split(jnp.concatenate(left_t, 0))
                th[h, kb, :, cols] = hi
                tl[h, kb, :, cols] = lo
                hi, lo = split(jnp.concatenate(right_t, 0))
                th[h, kb, :, right] = hi
                tl[h, kb, :, right] = lo

    def split_x(t):
        @pl.loop(0, 8)
        def _(b):
            rows = pl.ds(pl.multiple_of(b * 128, 128), 128)
            for part in range(2):
                hi, lo = split(xf[t, part, rows, :])
                dst = pl.ds(pl.multiple_of(part * F + b * 128, 128), 128)
                xh[t, dst, :] = hi
                xl[t, dst, :] = lo

    def gen_cols():
        for b in range(4):
            jj = b * 256 + iota((1, 256), 1)
            cos, sin = cos_sin((col_of[...] * (coff[0] + jj)) & MASK)
            w = window(jj)
            ph[0, :, b * 256 : (b + 1) * 256] = w * cos
            ph[1, :, b * 256 : (b + 1) * 256] = -(w * sin)

        @pl.loop(0, 32)
        def _(b):
            n = b * 32 + iota((32, 1), 0)
            m = (iota((1, M), 1) * (coff[0] + n)) & MASK
            cos, sin = cos_sin(m)
            hi, lo = split(jnp.concatenate([cos, -sin], 1))
            rows = pl.ds(pl.multiple_of(b * 32, 32), 32)
            eh[rows, :] = hi
            el[rows, :] = lo

    def matmul(u):
        h, t = divmod(u, NT)
        for half in range(2):
            rows = slice(8 * half, 8 * half + 8)
            out = dot3(
                th[h, rows].reshape(256, 2 * F), tl[h, rows].reshape(256, 2 * F), xh[t], xl[t]
            )
            s[u, half] = out.reshape(2, 2, 2, 4, 8, CW)

    def d2d(u):
        return pltpu.make_async_remote_copy(
            src_ref=s.at[u, 1 - core],
            dst_ref=rd.at[u],
            send_sem=d_ssem.at[u],
            recv_sem=d_rsem.at[u],
            device_id=(i ^ 1, j),
            device_id_type=MESH,
        )

    def region(order, k, c0, n, other):
        sel = [slice(None)] * 3
        for d in order[:k]:
            sel[d] = own[d]
        sel[order[k]] = 1 - own[order[k]] if other else own[order[k]]
        return (*sel, slice(c0, c0 + n))

    def exchange(u, k, gi):
        order, c0, n = groups_of(u)[gi]
        return pltpu.make_async_remote_copy(
            src_ref=s.at[(u, core, *region(order, k, c0, n, True))],
            dst_ref=recv_bufs[k].at[(u, *[slice(None)] * (2 - k), slice(c0, c0 + n))],
            send_sem=e_ssem.at[u, k, gi],
            recv_sem=e_rsem.at[u, k, gi],
            device_id=(i ^ FLIP[order[k]], j),
            device_id_type=MESH,
        )

    def finish_d2d(u):
        d2d(u).wait_recv()
        s[u, core] += rd[u]
        for gi in range(3):
            exchange(u, 0, gi).start()

    def finish_exchange(u, k):
        for gi, (order, c0, n) in enumerate(groups_of(u)):
            exchange(u, k, gi).wait_recv()
            at = (u, core, *region(order, k, c0, n, False))
            s[at] += recv_bufs[k][(u, *[slice(None)] * (2 - k), slice(c0, c0 + n))]
            if k < 2:
                exchange(u, k + 1, gi).start()

    sign = jnp.where(iota((8, 1), 0) < 4, -1.0, 1.0).astype(f32)

    def columns(u):
        h, t = divmod(u, NT)
        cols = slice(t * CW, (t + 1) * CW)
        for c in range(4):
            tile = s[u, core, own[0], own[1], own[2], c]
            fb[0, c] = tile
            fb[1, c] = jnp.concatenate([tile[4:], tile[:4]], 0) * sign
        for q0 in range(0, SLOTS, 4):
            tiles = []
            for q in range(q0, q0 + 4):
                st = strip_of[0, q]
                tiles.append(fb[0, st] * ph[0, q : q + 1, cols] + fb[1, st] * ph[1, q : q + 1, cols])
            hi, lo = split(jnp.concatenate(tiles, 0))
            ah[q0 * 8 : (q0 + 4) * 8, :] = hi
            al[q0 * 8 : (q0 + 4) * 8, :] = lo
        prod = dot3(ah[...], al[...], eh[cols, :], el[cols, :])
        if t == 0:
            gacc[...] = prod
        elif t < NT - 1:
            gacc[...] += prod
        else:
            total = (gacc[...] + prod).reshape(SLOTS, 8, 2 * M)
            cross = total[:, :, M:]
            cross = jnp.concatenate([cross[:, 4:], cross[:, :4]], 1)
            g[h] = total[:, :, :M] + cross * sign

    def a_copy(h, a):
        return pltpu.make_async_remote_copy(
            src_ref=g.at[h, pl.ds(3 * a, 3)],
            dst_ref=ra.at[h, xhi, kz],
            send_sem=a_ssem.at[h, a],
            recv_sem=a_rsem.at[h, xhi, kz],
            device_id=(a, z * 2 + core),
            device_id_type=MESH,
        )

    def start_a(h):
        for d in range(15, 0, -1):
            a_copy(h, i ^ d).start()

        @pl.when(core != xhi)
        def _():
            a_copy(h, i).start()

        @pl.when(core == xhi)
        def _():
            ra[h, xhi, kz] = g[h, pl.ds(3 * i, 3)]

    def end_a(h):
        for d in range(15, 0, -1):
            a_copy(h, i ^ d).wait_send()

        @pl.when(core != xhi)
        def _():
            a_copy(h, i).wait_send()

    def b_copy(h, k):
        return pltpu.make_async_remote_copy(
            src_ref=pb.at[h, k],
            dst_ref=rb.at[h, z],
            send_sem=b_ssem.at[h, k],
            recv_sem=b_rsem.at[h, z],
            device_id=(i, k * 2 + xhi),
            device_id_type=MESH,
        )

    def a_arrival(h, xs, k):
        return pltpu.make_async_remote_copy(
            src_ref=g.at[h, pl.ds(0, 3)],
            dst_ref=ra.at[h, xs, k],
            send_sem=a_ssem.at[h, 0],
            recv_sem=a_rsem.at[h, xs, k],
            device_id=(i, j),
            device_id_type=MESH,
        )

    def b_arrival(h, zs):
        return pltpu.make_async_remote_copy(
            src_ref=pb.at[h, 0],
            dst_ref=rb.at[h, zs],
            send_sem=b_ssem.at[h, 0],
            recv_sem=b_rsem.at[h, zs],
            device_id=(i, j),
            device_id_type=MESH,
        )

    def finish_a(h):
        for d in (1, 2, 3, 4, 5, 6, 7, 0):
            k = z ^ d
            a_arrival(h, 1 - xhi, k).wait_recv()

            @pl.when(jnp.logical_or(core != xhi, k != kz))
            def _():
                a_arrival(h, xhi, k).wait_recv()

            pb[h, k] = ra[h, 0, k] + ra[h, 1, k]
            if d:
                b_copy(h, k).start()

    def finish_b(h):
        total = pb[h, z]
        for d in range(1, 8):
            b_arrival(h, z ^ d).wait_recv()
            total = total + rb[h, z ^ d]
        out_ref[:, 0, 4 * h : 4 * h + 4, :] = total[:, :4]
        out_ref[:, 1, 4 * h : 4 * h + 4, :] = total[:, 4:]

    def end_b(h):
        for d in range(1, 8):
            b_copy(h, z ^ d).wait_send()

    def end_strips():
        for u in range(2 * NT):
            d2d(u).wait_send()
            for k in range(3):
                for gi in range(3):
                    exchange(u, k, gi).wait_send()

    def first_product():
        x_copy(0).wait()
        split_x(0)
        matmul(0)
        wait_barrier()
        d2d(0).start()

    def product(u):
        if 0 < u < NT:
            x_copy(u).wait()
            split_x(u)
        if u == NT:
            gen_t(1)
        matmul(u)
        d2d(u).start()

    def last_tables():
        strip_copy().wait()
        gen_cols()

    steps = {"d": finish_d2d, "c": columns, "a": finish_a, "s": start_a, "m": product}
    gen_slots()
    strip_copy().start()
    gen_u()
    gen_t(0)
    first_product()
    for kind, u in plan():
        if kind == "g":
            last_tables()
        elif kind == "e":
            finish_exchange(*u)
        elif kind == "b":
            finish_b(u)
        else:
            steps[kind](u)
    end_strips()
    end_a(0)
    end_b(0)
    finish_a(1)
    end_a(1)
    finish_b(1)
    end_b(1)


def plan():
    wire = {"d": 1.6, 0: 3.0, 1: 2.6, 2: 2.3}
    now, out, pending, ready = 0.0, [], [("d", 0, 1.6)], []
    todo = list(range(1, 2 * NT))
    tables = False
    while todo or pending or ready:
        due = sorted((t, k, u) for k, u, t in pending if t <= now)
        if due:
            t, kind, u = due[0]
            pending.remove((kind, u, t))
            out.append((kind, u))
            if kind == "d":
                pending.append(("e", (u, 0), now + 0.1 + wire[0]))
            elif kind == "e":
                u, k = u
                if k < 2:
                    pending.append(("e", (u, k + 1), now + 0.1 + wire[k + 1]))
                else:
                    ready.append(u)
            elif kind == "a":
                pending.append(("b", u, now + 6.5))
            now += 0.1
        elif ready:
            if not tables:
                tables = True
                out.append(("g", 0))
                now += 1.5
            u = ready.pop(0)
            out.append(("c", u))
            now += 0.35
            if u % NT == NT - 1:
                out.append(("s", u // NT))
                now += 0.25
                if u // NT == 0:
                    pending.append(("a", 0, now + 5.5))
        elif todo:
            u = todo.pop(0)
            out.append(("m", u))
            now += 1.75 + (0.3 if u < NT else 0) + (1.05 if u == NT else 0)
            pending.append(("d", u, now + wire["d"]))
        else:
            if not tables:
                tables = True
                out.append(("g", 0))
                now += 1.5
            now = max(now, min(t for _, _, t in pending))
    return out


def per_device(facets, row_off, col_off, strip_offset, subgrid_strip, subgrid_column, subgrid_slot):
    smem = pl.BlockSpec(memory_space=pltpu.SMEM)
    vmem = pl.BlockSpec(memory_space=pltpu.VMEM)
    dma = pltpu.SemaphoreType.DMA
    u = 2 * NT
    return pl.pallas_call(
        kernel,
        out_shape=jax.ShapeDtypeStruct((3, 2, 8, M), f32),
        in_specs=[pl.BlockSpec(memory_space=pl.ANY)] + [smem] * 6,
        out_specs=vmem,
        scratch_shapes=[
            pltpu.VMEM((1, 128), jnp.int32),
            pltpu.SMEM((1, 128), jnp.int32),
            pltpu.VMEM((SLOTS, 1), jnp.int32),
            pltpu.VMEM((NT, 2, F, CW), f32),
            pltpu.VMEM((NT, 2 * F, CW), bf16),
            pltpu.VMEM((NT, 2 * F, CW), bf16),
            pltpu.VMEM((2, 16, 32, 2 * F), bf16),
            pltpu.VMEM((2, 16, 32, 2 * F), bf16),
            pltpu.VMEM((2, 64, F), f32),
            pltpu.VMEM((2, 8, F), f32),
            pltpu.VMEM((u, 2, 2, 2, 2, 4, 8, CW), f32),
            pltpu.VMEM((u, 2, 2, 2, 4, 8, CW), f32),
            pltpu.VMEM((u, 2, 2, 4, 8, CW), f32),
            pltpu.VMEM((u, 2, 4, 8, CW), f32),
            pltpu.VMEM((u, 4, 8, CW), f32),
            pltpu.VMEM((2, 4, 8, CW), f32),
            pltpu.VMEM((2, SLOTS, F), f32),
            pltpu.VMEM((F, 2 * M), bf16),
            pltpu.VMEM((F, 2 * M), bf16),
            pltpu.VMEM((SLOTS * 8, CW), bf16),
            pltpu.VMEM((SLOTS * 8, CW), bf16),
            pltpu.VMEM((SLOTS * 8, 2 * M), f32),
            pltpu.VMEM((2, SLOTS, 8, M), f32),
            pltpu.VMEM((2, 2, 8, 3, 8, M), f32),
            pltpu.VMEM((2, 8, 3, 8, M), f32),
            pltpu.VMEM((2, 8, 3, 8, M), f32),
            dma((NT,)),
            dma((1,)),
            dma((u,)),
            dma((u,)),
            dma((u, 3, 3)),
            dma((u, 3, 3)),
            dma((2, 16)),
            dma((2, 2, 8)),
            dma((2, 8)),
            dma((2, 8)),
        ],
        compiler_params=pltpu.CompilerParams(
            collective_id=0, has_side_effects=True, vmem_limit_bytes=56 * 1024 * 1024
        ),
        name="facet_to_subgrid",
    )(facets, row_off, col_off, strip_offset, subgrid_strip, subgrid_column, subgrid_slot)


def solution(mesh):
    placed = (P(None, "frow", "fcol"), P("frow"), P("fcol"), P(), P(), P(), P())
    return jax.shard_map(
        per_device,
        mesh=mesh,
        in_specs=placed,
        out_specs=P("frow", None, "fcol", None),
        check_vma=False,
    )
```

```python
import math

import jax
import jax.numpy as jnp
from jax import lax
from jax.experimental import pallas as pl
from jax.experimental.pallas import tpu as pltpu
from jax.sharding import PartitionSpec as P

F = 1024
M = 128
N = 16384
MASK = N - 1
SLOTS = 48
CW = 256
NT = F // CW
f32 = jnp.float32
bf16 = jnp.bfloat16
MESH = pl.DeviceIdType.MESH

FLIP = (8, 2, 6)
ORDERS = ((0, 1, 2), (1, 2, 0), (2, 0, 1))


def groups_of(u):
    cuts = ((0, 2), (2, 1), (3, 1))
    return [(ORDERS[(u + g) % 3], c0, n) for g, (c0, n) in enumerate(cuts)]


def iota(shape, dim):
    return lax.broadcasted_iota(jnp.int32, shape, dim)


def cos_sin(m):
    q = (m + N // 8) >> 12
    x = (m - (q << 12)).astype(f32) * (2.0 * math.pi / N)
    x2 = x * x
    s = x * (1.0 + x2 * (-1.0 / 6 + x2 * (1.0 / 120 + x2 * (-1.0 / 5040 + x2 * (1.0 / 362880)))))
    c = 1.0 + x2 * (-0.5 + x2 * (1.0 / 24 + x2 * (-1.0 / 720 + x2 * (1.0 / 40320))))
    swap = (q & 1) == 1
    cos = jnp.where(swap, s, c)
    sin = jnp.where(swap, c, s)
    cos = jnp.where(((q + 1) & 2) == 2, -cos, cos)
    sin = jnp.where((q & 2) == 2, -sin, sin)
    return cos, sin


def window(j):
    x = (jnp.minimum(j, F - 1 - j).astype(f32) + 0.5) * (math.pi / F)
    x2 = x * x
    poly = 1.0 / 6227020800
    for k in (-39916800, 362880, -5040, 120, -6, 1):
        poly = poly * x2 + 1.0 / k
    return poly * x * (1.0 / math.sqrt(N))


def split(x):
    hi = x.astype(bf16)
    return hi, (x - hi.astype(f32)).astype(bf16)


def dot3(ah, al, bh, bl):
    def d(a, b):
        return jnp.dot(a, b, preferred_element_type=f32)

    return d(ah, bh) + d(ah, bl) + d(al, bh)


def kernel(
    x_hbm, *rest,
):
    scalars, (out_ref, *rest) = rest[:6], rest[6:]
    (roff, coff, soff, g_strip, g_column, g_slot), rest = rest[:6], rest[6:]
    body(x_hbm, scalars, roff, coff, soff, g_strip, g_column, g_slot, out_ref, *rest)


def body(
    x_hbm, scalars, roff, coff, soff, g_strip, g_column, g_slot, out_ref,
    strip_row, strip_of, col_of, xf, xh, xl, th, tl, ut, vt, s, rd, r0, r1, r2,
    fb, ph, eh, el, ah, al, gacc, g, ra, pb, rb,
    x_sem, st_sem, in_sem, d_ssem, d_rsem, e_ssem, e_rsem, a_ssem, a_rsem, b_ssem, b_rsem,
):
    i = lax.axis_index("frow")
    j = lax.axis_index("fcol")
    core = i & 1
    y = (i >> 1) & 3
    xlo = i >> 3
    z = j >> 1
    xhi = j & 1
    own = (xlo, (y ^ (y >> 1)) & 1, y >> 1)
    kz = own[0] * 4 + own[1] * 2 + own[2]
    recv_bufs = (r0, r1, r2)

    def x_copy(t):
        return pltpu.make_async_copy(
            x_hbm.at[:, :, pl.ds(t * CW, CW)], xf.at[t], x_sem.at[t]
        )

    def scalar_copies():
        for n, (src, dst) in enumerate(zip(scalars, (roff, coff, soff, g_strip, g_column, g_slot))):
            yield pltpu.make_async_copy(src, dst, in_sem.at[n])

    for copy in scalar_copies():
        copy.start()
    for t in range(NT):
        x_copy(t).start()

    barrier = pltpu.get_barrier_semaphore()

    def hello(fr, fc):
        pl.semaphore_signal(barrier, inc=1, device_id=(fr, fc), device_id_type=MESH)

    for flip in (1, *FLIP):
        hello(i ^ flip, j)

    for d in range(1, 16):
        hello((((i >> 1) ^ (d >> 1)) << 1) | xhi, z * 2 + (xhi ^ (d & 1)))

    @pl.when(core != xhi)
    def _():
        hello(i ^ 1, j)

    for d in range(1, 8):
        hello(i, (z ^ d) * 2 + xhi)

    def wait_barrier():
        pl.semaphore_wait(barrier, 27 - (1 - (core ^ xhi)))

    def gen_slots():
        lane = iota((1, 128), 1)
        row = iota((SLOTS, 1), 0)
        strips = jnp.zeros((1, 128), jnp.int32)
        columns_ = jnp.zeros((SLOTS, 1), jnp.int32)
        for n in range(SLOTS):
            strips = jnp.where(lane == g_slot[n], g_strip[n], strips)
            columns_ = jnp.where(row == g_slot[n], g_column[n], columns_)
        strip_row[...] = strips
        col_of[...] = columns_

    def strip_copy():
        return pltpu.make_async_copy(strip_row, strip_of, st_sem.at[0])

    def gen_u():
        row = iota((64, 1), 0)
        c = row & 3
        kb = row >> 2
        block = ((kb & 7) << 1) | (kb >> 3)
        f = jnp.where(c == 0, soff[0], jnp.where(c == 1, soff[1], jnp.where(c == 2, soff[2], soff[3])))
        f = f + 8 * block
        for b in range(4):
            p = roff[0] + b * 256 + iota((1, 256), 1)
            cos, sin = cos_sin((f * p) & MASK)
            ut[0, :, b * 256 : (b + 1) * 256] = cos
            ut[1, :, b * 256 : (b + 1) * 256] = sin

    def gen_v(h):
        r = iota((8, 1), 0)
        jj = iota((1, F), 1)
        m = ((r & 3) + 4 * h) * (roff[0] + jj) + (r >> 2) * (N // 4)
        cos, sin = cos_sin(m & MASK)
        w = window(jj)
        vt[0] = w * cos
        vt[1] = w * sin

    def gen_t(h, blocks):
        for b in range(4):
            cols = slice(b * 256, (b + 1) * 256)
            right = slice(F + b * 256, F + (b + 1) * 256)
            vr = vt[0, :, cols]
            vi = vt[1, :, cols]
            for kb in blocks:
                left_t, right_t = [], []
                for c in range(4):
                    q = kb * 4 + c
                    ur = ut[0, q : q + 1, cols]
                    ui = ut[1, q : q + 1, cols]
                    left_t.append(ur * vr - ui * vi)
                    right_t.append(ui * vr + ur * vi)
                hi, lo = split(jnp.concatenate(left_t, 0))
                th[h, kb, :, cols] = hi
                tl[h, kb, :, cols] = lo
                hi, lo = split(jnp.concatenate(right_t, 0))
                th[h, kb, :, right] = hi
                tl[h, kb, :, right] = lo

    def split_x(t):
        for part in range(2):
            for b in range(0, F, 128):
                hi, lo = split(xf[t, part, b : b + 128, :])
                xh[t, part * F + b : part * F + b + 128, :] = hi
                xl[t, part * F + b : part * F + b + 128, :] = lo

    def gen_cols():
        for b in range(4):
            jj = b * 256 + iota((1, 256), 1)
            cos, sin = cos_sin((col_of[...] * (coff[0] + jj)) & MASK)
            w = window(jj)
            ph[0, :, b * 256 : (b + 1) * 256] = w * cos
            ph[1, :, b * 256 : (b + 1) * 256] = -(w * sin)

        @pl.loop(0, 32)
        def _(b):
            n = b * 32 + iota((32, 1), 0)
            m = (iota((1, M), 1) * (coff[0] + n)) & MASK
            cos, sin = cos_sin(m)
            hi, lo = split(jnp.concatenate([cos, -sin], 1))
            rows = pl.ds(pl.multiple_of(b * 32, 32), 32)
            eh[rows, :] = hi
            el[rows, :] = lo

    def matmul(u, half):
        h, t = divmod(u, NT)
        rows = slice(8 * half, 8 * half + 8)
        out = dot3(
            th[h, rows].reshape(256, 2 * F), tl[h, rows].reshape(256, 2 * F), xh[t], xl[t]
        )
        s[u, half] = out.reshape(2, 2, 2, 4, 8, CW)

    def matmul_of(u, owner):
        h, t = divmod(u, NT)
        for x in range(2):
            rows = pl.ds(8 * owner + 4 * x, 4)
            out = dot3(
                th[h, rows].reshape(128, 2 * F), tl[h, rows].reshape(128, 2 * F), xh[t], xl[t]
            )
            s[u, owner, x] = out.reshape(2, 2, 4, 8, CW)

    def d2d(u):
        return pltpu.make_async_remote_copy(
            src_ref=s.at[u, 1 - core],
            dst_ref=rd.at[u],
            send_sem=d_ssem.at[u],
            recv_sem=d_rsem.at[u],
            device_id=(i ^ 1, j),
            device_id_type=MESH,
        )

    def region(order, k, c0, n, other):
        sel = [slice(None)] * 3
        for d in order[:k]:
            sel[d] = own[d]
        sel[order[k]] = 1 - own[order[k]] if other else own[order[k]]
        return (*sel, slice(c0, c0 + n))

    def exchange(u, k, gi):
        order, c0, n = groups_of(u)[gi]
        return pltpu.make_async_remote_copy(
            src_ref=s.at[(u, core, *region(order, k, c0, n, True))],
            dst_ref=recv_bufs[k].at[(u, *[slice(None)] * (2 - k), slice(c0, c0 + n))],
            send_sem=e_ssem.at[u, k, gi],
            recv_sem=e_rsem.at[u, k, gi],
            device_id=(i ^ FLIP[order[k]], j),
            device_id_type=MESH,
        )

    def finish_d2d(u):
        d2d(u).wait_recv()
        s[u, core] += rd[u]
        for gi in range(3):
            exchange(u, 0, gi).start()

    def finish_exchange(u, k):
        for gi, (order, c0, n) in enumerate(groups_of(u)):
            exchange(u, k, gi).wait_recv()
            at = (u, core, *region(order, k, c0, n, False))
            s[at] += recv_bufs[k][(u, *[slice(None)] * (2 - k), slice(c0, c0 + n))]
            if k < 2:
                exchange(u, k + 1, gi).start()

    sign = jnp.where(iota((8, 1), 0) < 4, -1.0, 1.0).astype(f32)

    def columns(u):
        h, t = divmod(u, NT)
        cols = slice(t * CW, (t + 1) * CW)
        for c in range(4):
            tile = s[u, core, own[0], own[1], own[2], c]
            fb[0, c] = tile
            fb[1, c] = jnp.concatenate([tile[4:], tile[:4]], 0) * sign
        for q0 in range(0, SLOTS, 4):
            tiles = []
            for q in range(q0, q0 + 4):
                st = strip_of[0, q]
                tiles.append(fb[0, st] * ph[0, q : q + 1, cols] + fb[1, st] * ph[1, q : q + 1, cols])
            hi, lo = split(jnp.concatenate(tiles, 0))
            ah[q0 * 8 : (q0 + 4) * 8, :] = hi
            al[q0 * 8 : (q0 + 4) * 8, :] = lo
        prod = dot3(ah[...], al[...], eh[cols, :], el[cols, :])
        if t == 0:
            gacc[...] = prod
        elif t < NT - 1:
            gacc[...] += prod
        else:
            total = (gacc[...] + prod).reshape(SLOTS, 8, 2 * M)
            cross = total[:, :, M:]
            cross = jnp.concatenate([cross[:, 4:], cross[:, :4]], 1)
            g[h] = total[:, :, :M] + cross * sign

    def a_copy(h, a):
        return pltpu.make_async_remote_copy(
            src_ref=g.at[h, pl.ds(3 * a, 3)],
            dst_ref=ra.at[h, xhi, kz],
            send_sem=a_ssem.at[h, a],
            recv_sem=a_rsem.at[h, xhi, kz],
            device_id=(a, z * 2 + core),
            device_id_type=MESH,
        )

    def start_a(h):
        for d in range(15, 0, -1):
            a_copy(h, i ^ d).start()

        @pl.when(core != xhi)
        def _():
            a_copy(h, i).start()

        @pl.when(core == xhi)
        def _():
            ra[h, xhi, kz] = g[h, pl.ds(3 * i, 3)]

    def end_a(h):
        for d in range(15, 0, -1):
            a_copy(h, i ^ d).wait_send()

        @pl.when(core != xhi)
        def _():
            a_copy(h, i).wait_send()

    def b_copy(h, k):
        return pltpu.make_async_remote_copy(
            src_ref=pb.at[h, k],
            dst_ref=rb.at[h, z],
            send_sem=b_ssem.at[h, k],
            recv_sem=b_rsem.at[h, z],
            device_id=(i, k * 2 + xhi),
            device_id_type=MESH,
        )

    def a_arrival(h, xs, k):
        return pltpu.make_async_remote_copy(
            src_ref=g.at[h, pl.ds(0, 3)],
            dst_ref=ra.at[h, xs, k],
            send_sem=a_ssem.at[h, 0],
            recv_sem=a_rsem.at[h, xs, k],
            device_id=(i, j),
            device_id_type=MESH,
        )

    def b_arrival(h, zs):
        return pltpu.make_async_remote_copy(
            src_ref=pb.at[h, 0],
            dst_ref=rb.at[h, zs],
            send_sem=b_ssem.at[h, 0],
            recv_sem=b_rsem.at[h, zs],
            device_id=(i, j),
            device_id_type=MESH,
        )

    def finish_a(h):
        for d in (1, 2, 3, 4, 5, 6, 7, 0):
            k = z ^ d
            a_arrival(h, 1 - xhi, k).wait_recv()

            @pl.when(jnp.logical_or(core != xhi, k != kz))
            def _():
                a_arrival(h, xhi, k).wait_recv()

            pb[h, k] = ra[h, 0, k] + ra[h, 1, k]
            if d:
                b_copy(h, k).start()

    def finish_b(h):
        total = pb[h, z]
        for d in range(1, 8):
            b_arrival(h, z ^ d).wait_recv()
            total = total + rb[h, z ^ d]
        out_ref[:, 0, 4 * h : 4 * h + 4, :] = total[:, :4]
        out_ref[:, 1, 4 * h : 4 * h + 4, :] = total[:, 4:]

    def end_b(h):
        for d in range(1, 8):
            b_copy(h, z ^ d).wait_send()

    def end_strips():
        for u in range(2 * NT):
            d2d(u).wait_send()
            for k in range(3):
                for gi in range(3):
                    exchange(u, k, gi).wait_send()

    last = 2 * NT - 1
    cuts = {1: range(0, 6), 2: range(6, 11), 3: range(11, 16)}

    def product(u):
        if u + 1 < NT:
            x_copy(u + 1).wait()
            split_x(u + 1)
        if u == 1:
            gen_v(1)
        if u in cuts:
            gen_t(1, cuts[u])
        if u < last:
            matmul(u, 0)
            matmul(u, 1)
            if u == 0:
                wait_barrier()
            d2d(u).start()
        else:
            matmul_of(u, 1 - core)
            d2d(u).start()
            matmul_of(u, core)

    for copy in scalar_copies():
        copy.wait()
    gen_slots()
    strip_copy().start()
    gen_u()
    gen_v(0)
    gen_t(0, range(16))
    x_copy(0).wait()
    split_x(0)
    for kind, *at in PLAN:
        if kind == "m":
            product(*at)
        elif kind == "d":
            finish_d2d(*at)
        elif kind == "e":
            finish_exchange(*at)
        elif kind == "g":
            strip_copy().wait()
            gen_cols()
        elif kind == "c":
            columns(*at)
        elif kind == "s":
            start_a(*at)
        elif kind == "w":
            end_strips()
        elif kind == "a":
            finish_a(*at)
        elif kind == "x":
            end_a(*at)
        elif kind == "b":
            finish_b(*at)
        elif kind == "y":
            end_b(*at)


PLAN = (
    ("m", 0),
    ("m", 1), ("d", 0),
    ("m", 2), ("d", 1),
    ("m", 3), ("e", 0, 0), ("d", 2),
    ("m", 4), ("e", 1, 0), ("d", 3), ("e", 0, 1),
    ("m", 5), ("e", 2, 0), ("d", 4), ("e", 1, 1),
    ("m", 6), ("e", 3, 0), ("d", 5), ("e", 0, 2), ("e", 2, 1),
    ("m", 7), ("e", 4, 0), ("d", 6), ("e", 1, 2), ("e", 3, 1), ("e", 5, 0), ("d", 7),
    ("e", 2, 2), ("g",), ("e", 4, 1), ("e", 6, 0), ("e", 3, 2), ("e", 5, 1), ("c", 0), ("c", 1), ("c", 2),
    ("e", 7, 0), ("e", 4, 2), ("e", 6, 1), ("e", 5, 2), ("c", 3), ("c", 4), ("c", 5),
    ("e", 7, 1), ("s", 0), ("e", 6, 2), ("c", 6),
    ("e", 7, 2), ("c", 7), ("s", 1), ("w",),
    ("a", 0), ("x", 0), ("a", 1), ("x", 1), ("b", 0), ("y", 0), ("b", 1), ("y", 1),
)


def per_device(facets, row_off, col_off, strip_offset, subgrid_strip, subgrid_column, subgrid_slot):
    vmem = pl.BlockSpec(memory_space=pltpu.VMEM)
    dma = pltpu.SemaphoreType.DMA
    u = 2 * NT
    return pl.pallas_call(
        kernel,
        out_shape=jax.ShapeDtypeStruct((3, 2, 8, M), f32),
        in_specs=[pl.BlockSpec(memory_space=pl.ANY)] * 7,
        out_specs=vmem,
        scratch_shapes=[
            *(pltpu.SMEM((n,), jnp.int32) for n in (1, 1, 4, SLOTS, SLOTS, SLOTS)),
            pltpu.VMEM((1, 128), jnp.int32),
            pltpu.SMEM((1, 128), jnp.int32),
            pltpu.VMEM((SLOTS, 1), jnp.int32),
            pltpu.VMEM((NT, 2, F, CW), f32),
            pltpu.VMEM((NT, 2 * F, CW), bf16),
            pltpu.VMEM((NT, 2 * F, CW), bf16),
            pltpu.VMEM((2, 16, 32, 2 * F), bf16),
            pltpu.VMEM((2, 16, 32, 2 * F), bf16),
            pltpu.VMEM((2, 64, F), f32),
            pltpu.VMEM((2, 8, F), f32),
            pltpu.VMEM((u, 2, 2, 2, 2, 4, 8, CW), f32),
            pltpu.VMEM((u, 2, 2, 2, 4, 8, CW), f32),
            pltpu.VMEM((u, 2, 2, 4, 8, CW), f32),
            pltpu.VMEM((u, 2, 4, 8, CW), f32),
            pltpu.VMEM((u, 4, 8, CW), f32),
            pltpu.VMEM((2, 4, 8, CW), f32),
            pltpu.VMEM((2, SLOTS, F), f32),
            pltpu.VMEM((F, 2 * M), bf16),
            pltpu.VMEM((F, 2 * M), bf16),
            pltpu.VMEM((SLOTS * 8, CW), bf16),
            pltpu.VMEM((SLOTS * 8, CW), bf16),
            pltpu.VMEM((SLOTS * 8, 2 * M), f32),
            pltpu.VMEM((2, SLOTS, 8, M), f32),
            pltpu.VMEM((2, 2, 8, 3, 8, M), f32),
            pltpu.VMEM((2, 8, 3, 8, M), f32),
            pltpu.VMEM((2, 8, 3, 8, M), f32),
            dma((NT,)),
            dma((1,)),
            dma((6,)),
            dma((u,)),
            dma((u,)),
            dma((u, 3, 3)),
            dma((u, 3, 3)),
            dma((2, 16)),
            dma((2, 2, 8)),
            dma((2, 8)),
            dma((2, 8)),
        ],
        compiler_params=pltpu.CompilerParams(
            collective_id=0, has_side_effects=True, vmem_limit_bytes=56 * 1024 * 1024
        ),
        name="facet_to_subgrid",
    )(facets, row_off, col_off, strip_offset, subgrid_strip, subgrid_column, subgrid_slot)


def solution(mesh):
    placed = (P(None, "frow", "fcol"), P("frow"), P("fcol"), P(), P(), P(), P())
    return jax.shard_map(
        per_device,
        mesh=mesh,
        in_specs=placed,
        out_specs=P("frow", None, "fcol", None),
        check_vma=False,
    )
```

```python
import math

import jax
import jax.numpy as jnp
from jax import lax
from jax.experimental import pallas as pl
from jax.experimental.pallas import tpu as pltpu
from jax.sharding import PartitionSpec as P

F = 1024
M = 128
N = 16384
MASK = N - 1
SLOTS = 48
CW = 256
NT = F // CW
LAST = 2 * NT - 1
f32 = jnp.float32
bf16 = jnp.bfloat16
MESH = pl.DeviceIdType.MESH

FLIP = (8, 2, 6)
ORDERS = ((0, 1, 2), (1, 2, 0), (2, 0, 1))


def flip_of(d):
    return (8 if d & 4 else 0) ^ (2 if d & 2 else 0) ^ (6 if d & 1 else 0)


def groups_of(u):
    cuts = ((0, 2), (2, 1), (3, 1))
    return [(ORDERS[(u + g) % 3], c0, n) for g, (c0, n) in enumerate(cuts)]


def iota(shape, dim):
    return lax.broadcasted_iota(jnp.int32, shape, dim)


def cos_sin(m):
    q = (m + N // 8) >> 12
    x = (m - (q << 12)).astype(f32) * (2.0 * math.pi / N)
    x2 = x * x
    s = x * (1.0 + x2 * (-1.0 / 6 + x2 * (1.0 / 120 + x2 * (-1.0 / 5040 + x2 * (1.0 / 362880)))))
    c = 1.0 + x2 * (-0.5 + x2 * (1.0 / 24 + x2 * (-1.0 / 720 + x2 * (1.0 / 40320))))
    swap = (q & 1) == 1
    cos = jnp.where(swap, s, c)
    sin = jnp.where(swap, c, s)
    cos = jnp.where(((q + 1) & 2) == 2, -cos, cos)
    sin = jnp.where((q & 2) == 2, -sin, sin)
    return cos, sin


def window(j):
    x = (jnp.minimum(j, F - 1 - j).astype(f32) + 0.5) * (math.pi / F)
    x2 = x * x
    poly = 1.0 / 6227020800
    for k in (-39916800, 362880, -5040, 120, -6, 1):
        poly = poly * x2 + 1.0 / k
    return poly * x * (1.0 / math.sqrt(N))


def split(x):
    hi = x.astype(bf16)
    return hi, (x - hi.astype(f32)).astype(bf16)


def dot3(ah, al, bh, bl):
    def d(a, b):
        return jnp.dot(a, b, preferred_element_type=f32)

    return d(ah, bh) + d(ah, bl) + d(al, bh)


def kernel(
    x_hbm, *rest,
):
    scalars, (out_ref, *rest) = rest[:6], rest[6:]
    (roff, coff, soff, g_strip, g_column, g_slot), rest = rest[:6], rest[6:]
    body(x_hbm, scalars, roff, coff, soff, g_strip, g_column, g_slot, out_ref, *rest)


def body(
    x_hbm, scalars, roff, coff, soff, g_strip, g_column, g_slot, out_ref,
    strip_row, strip_of, col_of, xf, xh, xl, th, tl, ut, vt, wt, s, rd, r0, r1, r2, r7,
    fb, ph, eh, el, ah, al, gacc, g, ra, pb, rb,
    x_sem, st_sem, in_sem, d_ssem, d_rsem, e_ssem, e_rsem, f_ssem, f_rsem, a_ssem, a_rsem, b_ssem, b_rsem,
):
    i = lax.axis_index("frow")
    j = lax.axis_index("fcol")
    core = i & 1
    y = (i >> 1) & 3
    xlo = i >> 3
    z = j >> 1
    xhi = j & 1
    own = (xlo, (y ^ (y >> 1)) & 1, y >> 1)
    kz = own[0] * 4 + own[1] * 2 + own[2]
    recv_bufs = (r0, r1, r2)

    def x_copy(t):
        return pltpu.make_async_copy(
            x_hbm.at[:, :, pl.ds(t * CW, CW)], xf.at[t], x_sem.at[t]
        )

    def scalar_copies():
        for n, (src, dst) in enumerate(zip(scalars, (roff, coff, soff, g_strip, g_column, g_slot))):
            yield pltpu.make_async_copy(src, dst, in_sem.at[n])

    for copy in scalar_copies():
        copy.start()
    for t in range(NT):
        x_copy(t).start()

    barrier = pltpu.get_barrier_semaphore()

    def hello(fr, fc):
        pl.semaphore_signal(barrier, inc=1, device_id=(fr, fc), device_id_type=MESH)

    for flip in (1, *(flip_of(d) for d in range(1, 8))):
        hello(i ^ flip, j)

    for d in range(1, 16):
        hello((((i >> 1) ^ (d >> 1)) << 1) | xhi, z * 2 + (xhi ^ (d & 1)))

    @pl.when(core != xhi)
    def _():
        hello(i ^ 1, j)

    for d in range(1, 8):
        hello(i, (z ^ d) * 2 + xhi)

    def wait_barrier():
        pl.semaphore_wait(barrier, 31 - (1 - (core ^ xhi)))

    def gen_slots():
        lane = iota((1, 128), 1)
        row = iota((SLOTS, 1), 0)
        strips = jnp.zeros((1, 128), jnp.int32)
        columns_ = jnp.zeros((SLOTS, 1), jnp.int32)
        for n in range(SLOTS):
            strips = jnp.where(lane == g_slot[n], g_strip[n], strips)
            columns_ = jnp.where(row == g_slot[n], g_column[n], columns_)
        strip_row[...] = strips
        col_of[...] = columns_

    def strip_copy():
        return pltpu.make_async_copy(strip_row, strip_of, st_sem.at[0])

    def gen_u():
        row = iota((64, 1), 0)
        c = row & 3
        kb = row >> 2
        block = ((kb & 7) << 1) | (kb >> 3)
        f = jnp.where(c == 0, soff[0], jnp.where(c == 1, soff[1], jnp.where(c == 2, soff[2], soff[3])))
        f = f + 8 * block
        for b in range(4):
            p = roff[0] + b * 256 + iota((1, 256), 1)
            cos, sin = cos_sin((f * p) & MASK)
            ut[0, :, b * 256 : (b + 1) * 256] = cos
            ut[1, :, b * 256 : (b + 1) * 256] = sin

    def gen_v(h):
        r = iota((8, 1), 0)
        jj = iota((1, F), 1)
        cos, sin = cos_sin((((r & 3) + 4 * h) * (roff[0] + jj)) & MASK)
        w = window(jj)
        vt[0] = w * cos
        vt[1] = w * sin

    def gen_t(h):
        first = iota((8, 1), 0) < 4
        for b in range(4):
            cols = slice(b * 256, (b + 1) * 256)
            vr = vt[0, :, cols]
            vi = vt[1, :, cols]
            for kb in range(16):
                tiles = [[], [], []]
                for c in (0, 2):
                    q = kb * 4 + c
                    ur = jnp.where(first, ut[0, q : q + 1, cols], ut[0, q + 1 : q + 2, cols])
                    ui = jnp.where(first, ut[1, q : q + 1, cols], ut[1, q + 1 : q + 2, cols])
                    re = ur * vr - ui * vi
                    im = -(ui * vr + ur * vi)
                    for tile, value in zip(tiles, (re, re + im, im - re)):
                        tile.append(value)
                for p in range(3):
                    hi, lo = split(jnp.concatenate(tiles[p], 0))
                    th[h, p, kb, :, cols] = hi
                    tl[h, p, kb, :, cols] = lo

    def split_x(t):
        @pl.loop(0, 8)
        def _(b):
            rows = pl.ds(pl.multiple_of(b * 128, 128), 128)
            re = xf[t, 0, rows, :]
            im = xf[t, 1, rows, :]
            for p, value in enumerate((re + im, im, re)):
                hi, lo = split(value)
                xh[t, p, rows, :] = hi
                xl[t, p, rows, :] = lo

    def gen_cols():
        for b in range(4):
            jj = b * 256 + iota((1, 256), 1)
            cos, sin = cos_sin((col_of[...] * (coff[0] + jj)) & MASK)
            w = window(jj)
            ph[0, :, b * 256 : (b + 1) * 256] = w * cos
            ph[1, :, b * 256 : (b + 1) * 256] = -(w * sin)

        lane = iota((1, M), 1)
        cos, sin = cos_sin((lane * (coff[0] + 8 * iota((F // 8, 1), 0))) & MASK)
        wt[0] = cos
        wt[1] = sin
        c1, s1 = cos_sin((lane * iota((8, 1), 0)) & MASK)

        @pl.loop(0, 16)
        def _(b):
            eight = pl.ds(pl.multiple_of(b * 8, 8), 8)
            wc = wt[0, eight, :]
            ws = wt[1, eight, :]
            for k in range(0, 8, 2):
                pair = []
                for n in (k, k + 1):
                    c0 = wc[n : n + 1]
                    s0 = ws[n : n + 1]
                    pair.append(jnp.concatenate([c0 * c1 - s0 * s1, -(s0 * c1 + c0 * s1)], 1))
                hi, lo = split(jnp.concatenate(pair, 0))
                rows = pl.ds(pl.multiple_of(b * 64 + k * 8, 16), 16)
                eh[rows, :] = hi
                el[rows, :] = lo

    def matmul(u, half):
        h, t = divmod(u, NT)
        rows = pl.ds(8 * half, 8)
        k1, k2, k3 = (
            dot3(
                th[h, p, rows].reshape(128, F), tl[h, p, rows].reshape(128, F), xh[t, p], xl[t, p]
            )
            for p in range(3)
        )
        re = (k1 - k2).reshape(2, 2, 2, 2, 8, CW)
        im = (k1 + k3).reshape(2, 2, 2, 2, 8, CW)
        for pair in range(2):
            s[u, half, :, :, :, 2 * pair] = re[:, :, :, pair]
            s[u, half, :, :, :, 2 * pair + 1] = im[:, :, :, pair]

    def d2d(u):
        return pltpu.make_async_remote_copy(
            src_ref=s.at[u, 1 - core],
            dst_ref=rd.at[u],
            send_sem=d_ssem.at[u],
            recv_sem=d_rsem.at[u],
            device_id=(i ^ 1, j),
            device_id_type=MESH,
        )

    def region(order, k, c0, n, other):
        sel = [slice(None)] * 3
        for d in order[:k]:
            sel[d] = own[d]
        sel[order[k]] = 1 - own[order[k]] if other else own[order[k]]
        return (*sel, slice(c0, c0 + n))

    def exchange(u, k, gi):
        order, c0, n = groups_of(u)[gi]
        return pltpu.make_async_remote_copy(
            src_ref=s.at[(u, core, *region(order, k, c0, n, True))],
            dst_ref=recv_bufs[k].at[(u, *[slice(None)] * (2 - k), slice(c0, c0 + n))],
            send_sem=e_ssem.at[u, k, gi],
            recv_sem=e_rsem.at[u, k, gi],
            device_id=(i ^ FLIP[order[k]], j),
            device_id_type=MESH,
        )

    def finish_d2d(u):
        d2d(u).wait_recv()
        s[u, core] += rd[u]
        if u == LAST:
            for d in range(1, 8):
                direct(d).start()
        else:
            for gi in range(3):
                exchange(u, 0, gi).start()

    def direct(d):
        to = (own[0] ^ (d >> 2), own[1] ^ ((d >> 1) & 1), own[2] ^ (d & 1))
        return pltpu.make_async_remote_copy(
            src_ref=s.at[(LAST, core, *to)],
            dst_ref=r7.at[d],
            send_sem=f_ssem.at[d],
            recv_sem=f_rsem.at[d],
            device_id=(i ^ flip_of(d), j),
            device_id_type=MESH,
        )

    def finish_direct():
        total = s[(LAST, core, *own)]
        for d in range(1, 8):
            direct(d).wait_recv()
            total = total + r7[d]
        s[(LAST, core, *own)] = total

    def finish_exchange(u, k):
        for gi, (order, c0, n) in enumerate(groups_of(u)):
            exchange(u, k, gi).wait_recv()
            at = (u, core, *region(order, k, c0, n, False))
            s[at] += recv_bufs[k][(u, *[slice(None)] * (2 - k), slice(c0, c0 + n))]
            if k < 2:
                exchange(u, k + 1, gi).start()

    sign = jnp.where(iota((8, 1), 0) < 4, -1.0, 1.0).astype(f32)

    def columns(u):
        h, t = divmod(u, NT)
        cols = slice(t * CW, (t + 1) * CW)
        for pair in range(2):
            re = s[u, core, own[0], own[1], own[2], 2 * pair]
            im = s[u, core, own[0], own[1], own[2], 2 * pair + 1]
            fb[0, 2 * pair] = jnp.concatenate([re[:4], im[:4]], 0)
            fb[1, 2 * pair] = jnp.concatenate([-im[:4], re[:4]], 0)
            fb[0, 2 * pair + 1] = jnp.concatenate([re[4:], im[4:]], 0)
            fb[1, 2 * pair + 1] = jnp.concatenate([-im[4:], re[4:]], 0)
        for q0 in range(0, SLOTS, 4):
            tiles = []
            for q in range(q0, q0 + 4):
                st = strip_of[0, q]
                tiles.append(fb[0, st] * ph[0, q : q + 1, cols] + fb[1, st] * ph[1, q : q + 1, cols])
            hi, lo = split(jnp.concatenate(tiles, 0))
            ah[q0 * 8 : (q0 + 4) * 8, :] = hi
            al[q0 * 8 : (q0 + 4) * 8, :] = lo
        prod = dot3(ah[...], al[...], eh[cols, :], el[cols, :])
        if t == 0:
            gacc[...] = prod
        elif t < NT - 1:
            gacc[...] += prod
        else:
            total = (gacc[...] + prod).reshape(SLOTS, 8, 2 * M)
            cross = total[:, :, M:]
            cross = jnp.concatenate([cross[:, 4:], cross[:, :4]], 1)
            g[h] = total[:, :, :M] + cross * sign

    def a_copy(h, a):
        return pltpu.make_async_remote_copy(
            src_ref=g.at[h, pl.ds(3 * a, 3)],
            dst_ref=ra.at[h, xhi, kz],
            send_sem=a_ssem.at[h, a],
            recv_sem=a_rsem.at[h, xhi, kz],
            device_id=(a, z * 2 + core),
            device_id_type=MESH,
        )

    def start_a(h):
        for d in range(15, 0, -1):
            a_copy(h, i ^ d).start()

        @pl.when(core != xhi)
        def _():
            a_copy(h, i).start()

        @pl.when(core == xhi)
        def _():
            ra[h, xhi, kz] = g[h, pl.ds(3 * i, 3)]

    def end_a(h):
        for d in range(15, 0, -1):
            a_copy(h, i ^ d).wait_send()

        @pl.when(core != xhi)
        def _():
            a_copy(h, i).wait_send()

    def b_copy(h, k):
        return pltpu.make_async_remote_copy(
            src_ref=pb.at[h, k],
            dst_ref=rb.at[h, z],
            send_sem=b_ssem.at[h, k],
            recv_sem=b_rsem.at[h, z],
            device_id=(i, k * 2 + xhi),
            device_id_type=MESH,
        )

    def a_arrival(h, xs, k):
        return pltpu.make_async_remote_copy(
            src_ref=g.at[h, pl.ds(0, 3)],
            dst_ref=ra.at[h, xs, k],
            send_sem=a_ssem.at[h, 0],
            recv_sem=a_rsem.at[h, xs, k],
            device_id=(i, j),
            device_id_type=MESH,
        )

    def b_arrival(h, zs):
        return pltpu.make_async_remote_copy(
            src_ref=pb.at[h, 0],
            dst_ref=rb.at[h, zs],
            send_sem=b_ssem.at[h, 0],
            recv_sem=b_rsem.at[h, zs],
            device_id=(i, j),
            device_id_type=MESH,
        )

    def finish_a(h):
        for d in (1, 2, 3, 4, 5, 6, 7, 0):
            k = z ^ d
            a_arrival(h, 1 - xhi, k).wait_recv()

            @pl.when(jnp.logical_or(core != xhi, k != kz))
            def _():
                a_arrival(h, xhi, k).wait_recv()

            pb[h, k] = ra[h, 0, k] + ra[h, 1, k]
            if d:
                b_copy(h, k).start()

    def finish_b(h):
        total = pb[h, z]
        for d in range(1, 8):
            b_arrival(h, z ^ d).wait_recv()
            total = total + rb[h, z ^ d]
        out_ref[:, 0, 4 * h : 4 * h + 4, :] = total[:, :4]
        out_ref[:, 1, 4 * h : 4 * h + 4, :] = total[:, 4:]

    def end_b(h):
        for d in range(1, 8):
            b_copy(h, z ^ d).wait_send()

    def end_strips():
        for d in range(1, 8):
            direct(d).wait_send()
        for u in range(2 * NT):
            d2d(u).wait_send()
            for k in range(3 if u < LAST else 0):
                for gi in range(3):
                    exchange(u, k, gi).wait_send()

    def product(u):
        if u < NT:
            x_copy(u).wait()
            split_x(u)
        if u < LAST:
            matmul(u, 0)
            matmul(u, 1)
            if u == 0:
                wait_barrier()
            d2d(u).start()
        else:
            matmul(u, 1 - core)
            d2d(u).start()
            matmul(u, core)

    for copy in scalar_copies():
        copy.wait()
    gen_slots()
    strip_copy().start()
    gen_u()
    gen_v(0)
    gen_t(0)
    for kind, *at in PLAN:
        if kind == "m":
            product(*at)
        elif kind == "d":
            finish_d2d(*at)
        elif kind == "e":
            finish_exchange(*at)
        elif kind == "f":
            finish_direct()
        elif kind == "t":
            gen_v(1)
            gen_t(1)
        elif kind == "g":
            strip_copy().wait()
            gen_cols()
        elif kind == "c":
            columns(*at)
        elif kind == "s":
            start_a(*at)
        elif kind == "w":
            end_strips()
        elif kind == "a":
            finish_a(*at)
        elif kind == "x":
            end_a(*at)
        elif kind == "b":
            finish_b(*at)
        elif kind == "y":
            end_b(*at)


PLAN = (
    ("m", 0),
    ("m", 1), ("d", 0),
    ("m", 2), ("d", 1),
    ("m", 3), ("d", 2), ("e", 0, 0),
    ("t",), ("d", 3),
    ("m", 4), ("e", 0, 1), ("e", 1, 0),
    ("m", 5), ("d", 4), ("e", 2, 0),
    ("m", 6), ("d", 5), ("e", 1, 1), ("e", 0, 2), ("e", 3, 0),
    ("m", 7), ("d", 6), ("e", 2, 1), ("e", 4, 0), ("e", 1, 2), ("d", 7),
    ("g",), ("e", 3, 1), ("e", 5, 0), ("e", 2, 2), ("c", 0), ("e", 4, 1), ("e", 6, 0), ("c", 1), ("e", 3, 2), ("c", 2),
    ("e", 5, 1), ("e", 4, 2), ("c", 3), ("e", 6, 1), ("s", 0), ("c", 4), ("e", 5, 2), ("c", 5), ("e", 6, 2), ("c", 6), ("w",),
    ("f",), ("c", 7), ("s", 1),
    ("a", 0), ("x", 0), ("a", 1), ("x", 1), ("b", 0), ("y", 0), ("b", 1), ("y", 1),
)


def per_device(facets, row_off, col_off, strip_offset, subgrid_strip, subgrid_column, subgrid_slot):
    vmem = pl.BlockSpec(memory_space=pltpu.VMEM)
    dma = pltpu.SemaphoreType.DMA
    u = 2 * NT
    return pl.pallas_call(
        kernel,
        out_shape=jax.ShapeDtypeStruct((3, 2, 8, M), f32),
        in_specs=[pl.BlockSpec(memory_space=pl.ANY)] * 7,
        out_specs=vmem,
        scratch_shapes=[
            *(pltpu.SMEM((n,), jnp.int32) for n in (1, 1, 4, SLOTS, SLOTS, SLOTS)),
            pltpu.VMEM((1, 128), jnp.int32),
            pltpu.SMEM((1, 128), jnp.int32),
            pltpu.VMEM((SLOTS, 1), jnp.int32),
            pltpu.VMEM((NT, 2, F, CW), f32),
            pltpu.VMEM((NT, 3, F, CW), bf16),
            pltpu.VMEM((NT, 3, F, CW), bf16),
            pltpu.VMEM((2, 3, 16, 16, F), bf16),
            pltpu.VMEM((2, 3, 16, 16, F), bf16),
            pltpu.VMEM((2, 64, F), f32),
            pltpu.VMEM((2, 8, F), f32),
            pltpu.VMEM((2, F // 8, M), f32),
            pltpu.VMEM((u, 2, 2, 2, 2, 4, 8, CW), f32),
            pltpu.VMEM((u, 2, 2, 2, 4, 8, CW), f32),
            pltpu.VMEM((u, 2, 2, 4, 8, CW), f32),
            pltpu.VMEM((u, 2, 4, 8, CW), f32),
            pltpu.VMEM((u, 4, 8, CW), f32),
            pltpu.VMEM((8, 4, 8, CW), f32),
            pltpu.VMEM((2, 4, 8, CW), f32),
            pltpu.VMEM((2, SLOTS, F), f32),
            pltpu.VMEM((F, 2 * M), bf16),
            pltpu.VMEM((F, 2 * M), bf16),
            pltpu.VMEM((SLOTS * 8, CW), bf16),
            pltpu.VMEM((SLOTS * 8, CW), bf16),
            pltpu.VMEM((SLOTS * 8, 2 * M), f32),
            pltpu.VMEM((2, SLOTS, 8, M), f32),
            pltpu.VMEM((2, 2, 8, 3, 8, M), f32),
            pltpu.VMEM((2, 8, 3, 8, M), f32),
            pltpu.VMEM((2, 8, 3, 8, M), f32),
            dma((NT,)),
            dma((1,)),
            dma((6,)),
            dma((u,)),
            dma((u,)),
            dma((u, 3, 3)),
            dma((u, 3, 3)),
            dma((8,)),
            dma((8,)),
            dma((2, 16)),
            dma((2, 2, 8)),
            dma((2, 8)),
            dma((2, 8)),
        ],
        compiler_params=pltpu.CompilerParams(
            collective_id=0, has_side_effects=True, vmem_limit_bytes=56 * 1024 * 1024
        ),
        name="facet_to_subgrid",
    )(facets, row_off, col_off, strip_offset, subgrid_strip, subgrid_column, subgrid_slot)


def solution(mesh):
    placed = (P(None, "frow", "fcol"), P("frow"), P("fcol"), P(), P(), P(), P())
    return jax.shard_map(
        per_device,
        mesh=mesh,
        in_specs=placed,
        out_specs=P("frow", None, "fcol", None),
        check_vma=False,
    )
```

```python
import math

import jax
import jax.numpy as jnp
from jax import lax
from jax.experimental import pallas as pl
from jax.experimental.pallas import tpu as pltpu
from jax.sharding import PartitionSpec as P

F = 1024
M = 128
N = 16384
MASK = N - 1
SLOTS = 48
CW = 256
NT = F // CW
LAST = 2 * NT - 1
PIECES = (7, 6, 5, 3, 4, 2, 1)
f32 = jnp.float32
bf16 = jnp.bfloat16
MESH = pl.DeviceIdType.MESH

FLIP = (8, 2, 6)
ORDERS = ((0, 1, 2), (1, 2, 0), (2, 0, 1))


def flip_of(d):
    return (8 if d & 4 else 0) ^ (2 if d & 2 else 0) ^ (6 if d & 1 else 0)


def groups_of(u):
    cuts = ((0, 2), (2, 1), (3, 1))
    return [(ORDERS[(u + g) % 3], c0, n) for g, (c0, n) in enumerate(cuts)]


def iota(shape, dim):
    return lax.broadcasted_iota(jnp.int32, shape, dim)


def cos_sin(m):
    q = (m + N // 8) >> 12
    x = (m - (q << 12)).astype(f32) * (2.0 * math.pi / N)
    x2 = x * x
    s = x * (1.0 + x2 * (-1.0 / 6 + x2 * (1.0 / 120 + x2 * (-1.0 / 5040 + x2 * (1.0 / 362880)))))
    c = 1.0 + x2 * (-0.5 + x2 * (1.0 / 24 + x2 * (-1.0 / 720 + x2 * (1.0 / 40320))))
    swap = (q & 1) == 1
    cos = jnp.where(swap, s, c)
    sin = jnp.where(swap, c, s)
    cos = jnp.where(((q + 1) & 2) == 2, -cos, cos)
    sin = jnp.where((q & 2) == 2, -sin, sin)
    return cos, sin


def window(j):
    x = (jnp.minimum(j, F - 1 - j).astype(f32) + 0.5) * (math.pi / F)
    x2 = x * x
    poly = 1.0 / 6227020800
    for k in (-39916800, 362880, -5040, 120, -6, 1):
        poly = poly * x2 + 1.0 / k
    return poly * x * (1.0 / math.sqrt(N))


def split(x):
    hi = x.astype(bf16)
    return hi, (x - hi.astype(f32)).astype(bf16)


def dot3(ah, al, bh, bl):
    def d(a, b):
        return jnp.dot(a, b, preferred_element_type=f32)

    return d(ah, bh) + d(ah, bl) + d(al, bh)


def kernel(
    x_hbm, *rest,
):
    scalars, (out_ref, *rest) = rest[:6], rest[6:]
    (roff, coff, soff, g_strip, g_column, g_slot), rest = rest[:6], rest[6:]
    body(x_hbm, scalars, roff, coff, soff, g_strip, g_column, g_slot, out_ref, *rest)


def body(
    x_hbm, scalars, roff, coff, soff, g_strip, g_column, g_slot, out_ref,
    strip_row, strip_of, col_of, xf, xh, xl, th, tl, ut, vt, wt, s, rd, r0, r1, r2, r7,
    fb, ph, eh, el, ah, al, gacc, g, ra, pb, rb,
    x_sem, st_sem, in_sem, d_ssem, d_rsem, e_ssem, e_rsem, f_ssem, f_rsem, a_ssem, a_rsem, b_ssem, b_rsem,
):
    i = lax.axis_index("frow")
    j = lax.axis_index("fcol")
    core = i & 1
    y = (i >> 1) & 3
    xlo = i >> 3
    z = j >> 1
    xhi = j & 1
    own = (xlo, (y ^ (y >> 1)) & 1, y >> 1)
    kz = own[0] * 4 + own[1] * 2 + own[2]
    recv_bufs = (r0, r1, r2)

    def x_copy(t):
        return pltpu.make_async_copy(
            x_hbm.at[:, :, pl.ds(t * CW, CW)], xf.at[t], x_sem.at[t]
        )

    def scalar_copies():
        for n, (src, dst) in enumerate(zip(scalars, (roff, coff, soff, g_strip, g_column, g_slot))):
            yield pltpu.make_async_copy(src, dst, in_sem.at[n])

    for copy in scalar_copies():
        copy.start()
    for t in range(NT):
        x_copy(t).start()

    barrier = pltpu.get_barrier_semaphore()

    def hello(fr, fc):
        pl.semaphore_signal(barrier, inc=1, device_id=(fr, fc), device_id_type=MESH)

    for flip in (1, *(flip_of(d) for d in range(1, 8))):
        hello(i ^ flip, j)

    for d in range(1, 16):
        hello((((i >> 1) ^ (d >> 1)) << 1) | xhi, z * 2 + (xhi ^ (d & 1)))

    @pl.when(core != xhi)
    def _():
        hello(i ^ 1, j)

    for d in range(1, 8):
        hello(i, (z ^ d) * 2 + xhi)

    def wait_barrier():
        pl.semaphore_wait(barrier, 31 - (1 - (core ^ xhi)))

    def gen_slots():
        lane = iota((1, 128), 1)
        row = iota((SLOTS, 1), 0)
        strips = jnp.zeros((1, 128), jnp.int32)
        columns_ = jnp.zeros((SLOTS, 1), jnp.int32)
        for n in range(SLOTS):
            strips = jnp.where(lane == g_slot[n], g_strip[n], strips)
            columns_ = jnp.where(row == g_slot[n], g_column[n], columns_)
        strip_row[...] = strips
        col_of[...] = columns_

    def strip_copy():
        return pltpu.make_async_copy(strip_row, strip_of, st_sem.at[0])

    def gen_u():
        row = iota((64, 1), 0)
        c = row & 3
        kb = row >> 2
        block = ((kb & 7) << 1) | (kb >> 3)
        f = jnp.where(c == 0, soff[0], jnp.where(c == 1, soff[1], jnp.where(c == 2, soff[2], soff[3])))
        f = f + 8 * block
        for b in range(4):
            p = roff[0] + b * 256 + iota((1, 256), 1)
            cos, sin = cos_sin((f * p) & MASK)
            ut[0, :, b * 256 : (b + 1) * 256] = cos
            ut[1, :, b * 256 : (b + 1) * 256] = sin

    def gen_v(h):
        r = iota((8, 1), 0)
        jj = iota((1, F), 1)
        cos, sin = cos_sin((((r & 3) + 4 * h) * (roff[0] + jj)) & MASK)
        w = window(jj)
        vt[0] = w * cos
        vt[1] = w * sin

    def gen_t(h):
        first = iota((8, 1), 0) < 4
        for b in range(4):
            cols = slice(b * 256, (b + 1) * 256)
            vr = vt[0, :, cols]
            vi = vt[1, :, cols]
            for kb in range(16):
                tiles = [[], [], []]
                for c in (0, 2):
                    q = kb * 4 + c
                    ur = jnp.where(first, ut[0, q : q + 1, cols], ut[0, q + 1 : q + 2, cols])
                    ui = jnp.where(first, ut[1, q : q + 1, cols], ut[1, q + 1 : q + 2, cols])
                    re = ur * vr - ui * vi
                    im = -(ui * vr + ur * vi)
                    for tile, value in zip(tiles, (re, re + im, im - re)):
                        tile.append(value)
                for p in range(3):
                    hi, lo = split(jnp.concatenate(tiles[p], 0))
                    th[h, p, kb, :, cols] = hi
                    tl[h, p, kb, :, cols] = lo

    def split_x(t):
        @pl.loop(0, 8)
        def _(b):
            rows = pl.ds(pl.multiple_of(b * 128, 128), 128)
            re = xf[t, 0, rows, :]
            im = xf[t, 1, rows, :]
            for p, value in enumerate((re + im, im, re)):
                hi, lo = split(value)
                xh[t, p, rows, :] = hi
                xl[t, p, rows, :] = lo

    def gen_cols():
        for b in range(4):
            jj = b * 256 + iota((1, 256), 1)
            cos, sin = cos_sin((col_of[...] * (coff[0] + jj)) & MASK)
            w = window(jj)
            ph[0, :, b * 256 : (b + 1) * 256] = w * cos
            ph[1, :, b * 256 : (b + 1) * 256] = -(w * sin)

        lane = iota((1, M), 1)
        cos, sin = cos_sin((lane * (coff[0] + 8 * iota((F // 8, 1), 0))) & MASK)
        wt[0] = cos
        wt[1] = sin
        c1, s1 = cos_sin((lane * iota((8, 1), 0)) & MASK)

        @pl.loop(0, 16)
        def _(b):
            eight = pl.ds(pl.multiple_of(b * 8, 8), 8)
            wc = wt[0, eight, :]
            ws = wt[1, eight, :]
            for k in range(0, 8, 2):
                pair = []
                for n in (k, k + 1):
                    c0 = wc[n : n + 1]
                    s0 = ws[n : n + 1]
                    pair.append(jnp.concatenate([c0 * c1 - s0 * s1, -(s0 * c1 + c0 * s1)], 1))
                hi, lo = split(jnp.concatenate(pair, 0))
                rows = pl.ds(pl.multiple_of(b * 64 + k * 8, 16), 16)
                eh[rows, :] = hi
                el[rows, :] = lo

    def matmul(u, half):
        h, t = divmod(u, NT)
        rows = pl.ds(8 * half, 8)
        k1, k2, k3 = (
            dot3(
                th[h, p, rows].reshape(128, F), tl[h, p, rows].reshape(128, F), xh[t, p], xl[t, p]
            )
            for p in range(3)
        )
        re = (k1 - k2).reshape(2, 2, 2, 2, 8, CW)
        im = (k1 + k3).reshape(2, 2, 2, 2, 8, CW)
        for pair in range(2):
            s[u, half, :, :, :, 2 * pair] = re[:, :, :, pair]
            s[u, half, :, :, :, 2 * pair + 1] = im[:, :, :, pair]

    def d2d(u):
        return pltpu.make_async_remote_copy(
            src_ref=s.at[u, 1 - core],
            dst_ref=rd.at[u],
            send_sem=d_ssem.at[u],
            recv_sem=d_rsem.at[u],
            device_id=(i ^ 1, j),
            device_id_type=MESH,
        )

    def region(order, k, c0, n, other):
        sel = [slice(None)] * 3
        for d in order[:k]:
            sel[d] = own[d]
        sel[order[k]] = 1 - own[order[k]] if other else own[order[k]]
        return (*sel, slice(c0, c0 + n))

    def exchange(u, k, gi):
        order, c0, n = groups_of(u)[gi]
        return pltpu.make_async_remote_copy(
            src_ref=s.at[(u, core, *region(order, k, c0, n, True))],
            dst_ref=recv_bufs[k].at[(u, *[slice(None)] * (2 - k), slice(c0, c0 + n))],
            send_sem=e_ssem.at[u, k, gi],
            recv_sem=e_rsem.at[u, k, gi],
            device_id=(i ^ FLIP[order[k]], j),
            device_id_type=MESH,
        )

    def finish_d2d(u):
        d2d(u).wait_recv()
        s[u, core] += rd[u]
        if u >= NT:
            for d in PIECES:
                direct(u, d).start()
        else:
            for gi in range(3):
                exchange(u, 0, gi).start()

    def direct(u, d):
        to = (own[0] ^ (d >> 2), own[1] ^ ((d >> 1) & 1), own[2] ^ (d & 1))
        return pltpu.make_async_remote_copy(
            src_ref=s.at[(u, core, *to)],
            dst_ref=r7.at[u - NT, d],
            send_sem=f_ssem.at[u - NT, d],
            recv_sem=f_rsem.at[u - NT, d],
            device_id=(i ^ flip_of(d), j),
            device_id_type=MESH,
        )

    def finish_direct(u):
        total = s[(u, core, *own)]
        for d in PIECES:
            direct(u, d).wait_recv()
            total = total + r7[u - NT, d]
        s[(u, core, *own)] = total

    def finish_exchange(u, k):
        for gi, (order, c0, n) in enumerate(groups_of(u)):
            exchange(u, k, gi).wait_recv()
            at = (u, core, *region(order, k, c0, n, False))
            s[at] += recv_bufs[k][(u, *[slice(None)] * (2 - k), slice(c0, c0 + n))]
            if k < 2:
                exchange(u, k + 1, gi).start()

    sign = jnp.where(iota((8, 1), 0) < 4, -1.0, 1.0).astype(f32)

    def columns(u):
        h, t = divmod(u, NT)
        cols = slice(t * CW, (t + 1) * CW)
        for pair in range(2):
            re = s[u, core, own[0], own[1], own[2], 2 * pair]
            im = s[u, core, own[0], own[1], own[2], 2 * pair + 1]
            fb[0, 2 * pair] = jnp.concatenate([re[:4], im[:4]], 0)
            fb[1, 2 * pair] = jnp.concatenate([-im[:4], re[:4]], 0)
            fb[0, 2 * pair + 1] = jnp.concatenate([re[4:], im[4:]], 0)
            fb[1, 2 * pair + 1] = jnp.concatenate([-im[4:], re[4:]], 0)
        for q0 in range(0, SLOTS, 4):
            tiles = []
            for q in range(q0, q0 + 4):
                st = strip_of[0, q]
                tiles.append(fb[0, st] * ph[0, q : q + 1, cols] + fb[1, st] * ph[1, q : q + 1, cols])
            hi, lo = split(jnp.concatenate(tiles, 0))
            ah[q0 * 8 : (q0 + 4) * 8, :] = hi
            al[q0 * 8 : (q0 + 4) * 8, :] = lo
        prod = dot3(ah[...], al[...], eh[cols, :], el[cols, :])
        if t == 0:
            gacc[...] = prod
        elif t < NT - 1:
            gacc[...] += prod
        else:
            total = (gacc[...] + prod).reshape(SLOTS, 8, 2 * M)
            cross = total[:, :, M:]
            cross = jnp.concatenate([cross[:, 4:], cross[:, :4]], 1)
            g[h] = total[:, :, :M] + cross * sign

    def a_copy(h, a):
        return pltpu.make_async_remote_copy(
            src_ref=g.at[h, pl.ds(3 * a, 3)],
            dst_ref=ra.at[h, xhi, kz],
            send_sem=a_ssem.at[h, a],
            recv_sem=a_rsem.at[h, xhi, kz],
            device_id=(a, z * 2 + core),
            device_id_type=MESH,
        )

    def start_a(h):
        for d in range(15, 0, -1):
            a_copy(h, i ^ d).start()

        @pl.when(core != xhi)
        def _():
            a_copy(h, i).start()

        @pl.when(core == xhi)
        def _():
            ra[h, xhi, kz] = g[h, pl.ds(3 * i, 3)]

    def end_a(h):
        for d in range(15, 0, -1):
            a_copy(h, i ^ d).wait_send()

        @pl.when(core != xhi)
        def _():
            a_copy(h, i).wait_send()

    def b_copy(h, k):
        return pltpu.make_async_remote_copy(
            src_ref=pb.at[h, k],
            dst_ref=rb.at[h, z],
            send_sem=b_ssem.at[h, k],
            recv_sem=b_rsem.at[h, z],
            device_id=(i, k * 2 + xhi),
            device_id_type=MESH,
        )

    def a_arrival(h, xs, k):
        return pltpu.make_async_remote_copy(
            src_ref=g.at[h, pl.ds(0, 3)],
            dst_ref=ra.at[h, xs, k],
            send_sem=a_ssem.at[h, 0],
            recv_sem=a_rsem.at[h, xs, k],
            device_id=(i, j),
            device_id_type=MESH,
        )

    def b_arrival(h, zs):
        return pltpu.make_async_remote_copy(
            src_ref=pb.at[h, 0],
            dst_ref=rb.at[h, zs],
            send_sem=b_ssem.at[h, 0],
            recv_sem=b_rsem.at[h, zs],
            device_id=(i, j),
            device_id_type=MESH,
        )

    def finish_a(h):
        for d in (1, 2, 3, 4, 5, 6, 7, 0):
            k = z ^ d
            a_arrival(h, 1 - xhi, k).wait_recv()

            @pl.when(jnp.logical_or(core != xhi, k != kz))
            def _():
                a_arrival(h, xhi, k).wait_recv()

            pb[h, k] = ra[h, 0, k] + ra[h, 1, k]
            if d:
                b_copy(h, k).start()

    def finish_b(h):
        total = pb[h, z]
        for d in range(1, 8):
            b_arrival(h, z ^ d).wait_recv()
            total = total + rb[h, z ^ d]
        out_ref[:, 0, 4 * h : 4 * h + 4, :] = total[:, :4]
        out_ref[:, 1, 4 * h : 4 * h + 4, :] = total[:, 4:]

    def end_b(h):
        for d in range(1, 8):
            b_copy(h, z ^ d).wait_send()

    def end_strips():
        for u in range(2 * NT):
            d2d(u).wait_send()
            for d in PIECES if u >= NT else ():
                direct(u, d).wait_send()
            for k in range(3 if u < NT else 0):
                for gi in range(3):
                    exchange(u, k, gi).wait_send()

    def product(u):
        if u < NT:
            x_copy(u).wait()
            split_x(u)
        if u < LAST:
            matmul(u, 0)
            matmul(u, 1)
            if u == 0:
                wait_barrier()
            d2d(u).start()
        else:
            matmul(u, 1 - core)
            d2d(u).start()
            matmul(u, core)

    for copy in scalar_copies():
        copy.wait()
    gen_slots()
    strip_copy().start()
    gen_u()
    gen_v(0)
    gen_t(0)
    for kind, *at in PLAN:
        if kind == "m":
            product(*at)
        elif kind == "d":
            finish_d2d(*at)
        elif kind == "e":
            finish_exchange(*at)
        elif kind == "f":
            finish_direct(*at)
        elif kind == "t":
            gen_v(1)
            gen_t(1)
        elif kind == "g":
            strip_copy().wait()
            gen_cols()
        elif kind == "c":
            columns(*at)
        elif kind == "s":
            start_a(*at)
        elif kind == "w":
            end_strips()
        elif kind == "a":
            finish_a(*at)
        elif kind == "x":
            end_a(*at)
        elif kind == "b":
            finish_b(*at)
        elif kind == "y":
            end_b(*at)


PLAN = (
    ("m", 0),
    ("m", 1), ("d", 0),
    ("m", 2), ("d", 1),
    ("m", 3), ("d", 2), ("e", 0, 0),
    ("t",), ("d", 3),
    ("m", 4), ("e", 1, 0),
    ("m", 5), ("d", 4), ("e", 0, 1), ("e", 2, 0), ("e", 3, 0),
    ("m", 6), ("d", 5), ("e", 1, 1),
    ("m", 7), ("d", 6), ("e", 2, 1), ("e", 3, 1), ("d", 7),
    ("g",), ("e", 0, 2), ("c", 0), ("e", 1, 2), ("c", 1), ("e", 2, 2), ("c", 2), ("e", 3, 2), ("c", 3), ("s", 0),
    ("f", 4), ("c", 4), ("f", 5), ("c", 5), ("f", 6), ("c", 6), ("w",), ("f", 7), ("c", 7), ("s", 1),
    ("a", 0), ("x", 0), ("a", 1), ("x", 1), ("b", 0), ("y", 0), ("b", 1), ("y", 1),
)


def per_device(facets, row_off, col_off, strip_offset, subgrid_strip, subgrid_column, subgrid_slot):
    vmem = pl.BlockSpec(memory_space=pltpu.VMEM)
    dma = pltpu.SemaphoreType.DMA
    u = 2 * NT
    return pl.pallas_call(
        kernel,
        out_shape=jax.ShapeDtypeStruct((3, 2, 8, M), f32),
        in_specs=[pl.BlockSpec(memory_space=pl.ANY)] * 7,
        out_specs=vmem,
        scratch_shapes=[
            *(pltpu.SMEM((n,), jnp.int32) for n in (1, 1, 4, SLOTS, SLOTS, SLOTS)),
            pltpu.VMEM((1, 128), jnp.int32),
            pltpu.SMEM((1, 128), jnp.int32),
            pltpu.VMEM((SLOTS, 1), jnp.int32),
            pltpu.VMEM((NT, 2, F, CW), f32),
            pltpu.VMEM((NT, 3, F, CW), bf16),
            pltpu.VMEM((NT, 3, F, CW), bf16),
            pltpu.VMEM((2, 3, 16, 16, F), bf16),
            pltpu.VMEM((2, 3, 16, 16, F), bf16),
            pltpu.VMEM((2, 64, F), f32),
            pltpu.VMEM((2, 8, F), f32),
            pltpu.VMEM((2, F // 8, M), f32),
            pltpu.VMEM((u, 2, 2, 2, 2, 4, 8, CW), f32),
            pltpu.VMEM((u, 2, 2, 2, 4, 8, CW), f32),
            pltpu.VMEM((NT, 2, 2, 4, 8, CW), f32),
            pltpu.VMEM((NT, 2, 4, 8, CW), f32),
            pltpu.VMEM((NT, 4, 8, CW), f32),
            pltpu.VMEM((NT, 8, 4, 8, CW), f32),
            pltpu.VMEM((2, 4, 8, CW), f32),
            pltpu.VMEM((2, SLOTS, F), f32),
            pltpu.VMEM((F, 2 * M), bf16),
            pltpu.VMEM((F, 2 * M), bf16),
            pltpu.VMEM((SLOTS * 8, CW), bf16),
            pltpu.VMEM((SLOTS * 8, CW), bf16),
            pltpu.VMEM((SLOTS * 8, 2 * M), f32),
            pltpu.VMEM((2, SLOTS, 8, M), f32),
            pltpu.VMEM((2, 2, 8, 3, 8, M), f32),
            pltpu.VMEM((2, 8, 3, 8, M), f32),
            pltpu.VMEM((2, 8, 3, 8, M), f32),
            dma((NT,)),
            dma((1,)),
            dma((6,)),
            dma((u,)),
            dma((u,)),
            dma((NT, 3, 3)),
            dma((NT, 3, 3)),
            dma((NT, 8)),
            dma((NT, 8)),
            dma((2, 16)),
            dma((2, 2, 8)),
            dma((2, 8)),
            dma((2, 8)),
        ],
        compiler_params=pltpu.CompilerParams(
            collective_id=0, has_side_effects=True, vmem_limit_bytes=56 * 1024 * 1024
        ),
        name="facet_to_subgrid",
    )(facets, row_off, col_off, strip_offset, subgrid_strip, subgrid_column, subgrid_slot)


def solution(mesh):
    placed = (P(None, "frow", "fcol"), P("frow"), P("fcol"), P(), P(), P(), P())
    return jax.shard_map(
        per_device,
        mesh=mesh,
        in_specs=placed,
        out_specs=P("frow", None, "fcol", None),
        check_vma=False,
    )
```

```python
import math

import jax
import jax.numpy as jnp
from jax import lax
from jax.experimental import pallas as pl
from jax.experimental.pallas import tpu as pltpu
from jax.sharding import PartitionSpec as P

F = 1024
M = 128
N = 16384
MASK = N - 1
SLOTS = 48
CW = 256
NT = F // CW
LAST = 2 * NT - 1
STEPPED = 3
PIECES = (7, 6, 5, 3, 4, 2, 1)
f32 = jnp.float32
bf16 = jnp.bfloat16
MESH = pl.DeviceIdType.MESH

FLIP = (8, 2, 6)
ORDERS = ((0, 1, 2), (1, 2, 0), (2, 0, 1))


def flip_of(d):
    return (8 if d & 4 else 0) ^ (2 if d & 2 else 0) ^ (6 if d & 1 else 0)


def groups_of(u):
    cuts = ((0, 2), (2, 1), (3, 1))
    return [(ORDERS[(u + g) % 3], c0, n) for g, (c0, n) in enumerate(cuts)]


def iota(shape, dim):
    return lax.broadcasted_iota(jnp.int32, shape, dim)


def cos_sin(m):
    q = (m + N // 8) >> 12
    x = (m - (q << 12)).astype(f32) * (2.0 * math.pi / N)
    x2 = x * x
    s = x * (1.0 + x2 * (-1.0 / 6 + x2 * (1.0 / 120 + x2 * (-1.0 / 5040 + x2 * (1.0 / 362880)))))
    c = 1.0 + x2 * (-0.5 + x2 * (1.0 / 24 + x2 * (-1.0 / 720 + x2 * (1.0 / 40320))))
    swap = (q & 1) == 1
    cos = jnp.where(swap, s, c)
    sin = jnp.where(swap, c, s)
    cos = jnp.where(((q + 1) & 2) == 2, -cos, cos)
    sin = jnp.where((q & 2) == 2, -sin, sin)
    return cos, sin


def window(j):
    x = (jnp.minimum(j, F - 1 - j).astype(f32) + 0.5) * (math.pi / F)
    x2 = x * x
    poly = 1.0 / 6227020800
    for k in (-39916800, 362880, -5040, 120, -6, 1):
        poly = poly * x2 + 1.0 / k
    return poly * x * (1.0 / math.sqrt(N))


def split(x):
    hi = x.astype(bf16)
    return hi, (x - hi.astype(f32)).astype(bf16)


def dot3(ah, al, bh, bl):
    def d(a, b):
        return jnp.dot(a, b, preferred_element_type=f32)

    return d(ah, bh) + d(ah, bl) + d(al, bh)


def kernel(
    x_hbm, *rest,
):
    scalars, (out_ref, *rest) = rest[:6], rest[6:]
    (roff, coff, soff, g_strip, g_column, g_slot), rest = rest[:6], rest[6:]
    body(x_hbm, scalars, roff, coff, soff, g_strip, g_column, g_slot, out_ref, *rest)


def body(
    x_hbm, scalars, roff, coff, soff, g_strip, g_column, g_slot, out_ref,
    strip_row, strip_of, col_of, xf, xh, xl, th, tl, ut, vt, wt, s, rd, r0, r1, r2, r7,
    fb, ph, eh, el, ah, al, gacc, g, ra, pb, rb,
    x_sem, st_sem, in_sem, d_ssem, d_rsem, e_ssem, e_rsem, f_ssem, f_rsem, a_ssem, a_rsem, b_ssem, b_rsem,
):
    i = lax.axis_index("frow")
    j = lax.axis_index("fcol")
    core = i & 1
    y = (i >> 1) & 3
    xlo = i >> 3
    z = j >> 1
    xhi = j & 1
    own = (xlo, (y ^ (y >> 1)) & 1, y >> 1)
    kz = own[0] * 4 + own[1] * 2 + own[2]
    recv_bufs = (r0, r1, r2)

    def x_copy(t):
        return pltpu.make_async_copy(
            x_hbm.at[:, :, pl.ds(t * CW, CW)], xf.at[t], x_sem.at[t]
        )

    def scalar_copies():
        for n, (src, dst) in enumerate(zip(scalars, (roff, coff, soff, g_strip, g_column, g_slot))):
            yield pltpu.make_async_copy(src, dst, in_sem.at[n])

    for copy in scalar_copies():
        copy.start()
    for t in range(NT):
        x_copy(t).start()

    barrier = pltpu.get_barrier_semaphore()

    def hello(fr, fc):
        pl.semaphore_signal(barrier, inc=1, device_id=(fr, fc), device_id_type=MESH)

    for flip in (1, *(flip_of(d) for d in range(1, 8))):
        hello(i ^ flip, j)

    for d in range(1, 16):
        hello((((i >> 1) ^ (d >> 1)) << 1) | xhi, z * 2 + (xhi ^ (d & 1)))

    @pl.when(core != xhi)
    def _():
        hello(i ^ 1, j)

    for d in range(1, 8):
        hello(i, (z ^ d) * 2 + xhi)

    def wait_barrier():
        pl.semaphore_wait(barrier, 31 - (1 - (core ^ xhi)))

    def gen_slots():
        lane = iota((1, 128), 1)
        row = iota((SLOTS, 1), 0)
        strips = jnp.zeros((1, 128), jnp.int32)
        columns_ = jnp.zeros((SLOTS, 1), jnp.int32)
        for n in range(SLOTS):
            strips = jnp.where(lane == g_slot[n], g_strip[n], strips)
            columns_ = jnp.where(row == g_slot[n], g_column[n], columns_)
        strip_row[...] = strips
        col_of[...] = columns_

    def strip_copy():
        return pltpu.make_async_copy(strip_row, strip_of, st_sem.at[0])

    def gen_u():
        row = iota((64, 1), 0)
        c = row & 3
        kb = row >> 2
        block = ((kb & 7) << 1) | (kb >> 3)
        f = jnp.where(c == 0, soff[0], jnp.where(c == 1, soff[1], jnp.where(c == 2, soff[2], soff[3])))
        f = f + 8 * block
        for b in range(4):
            p = roff[0] + b * 256 + iota((1, 256), 1)
            cos, sin = cos_sin((f * p) & MASK)
            ut[0, :, b * 256 : (b + 1) * 256] = cos
            ut[1, :, b * 256 : (b + 1) * 256] = sin

    def gen_v(h):
        r = iota((8, 1), 0)
        jj = iota((1, F), 1)
        cos, sin = cos_sin((((r & 3) + 4 * h) * (roff[0] + jj)) & MASK)
        w = window(jj)
        vt[0] = w * cos
        vt[1] = w * sin

    def gen_t(h):
        first = iota((8, 1), 0) < 4
        for b in range(4):
            cols = slice(b * 256, (b + 1) * 256)
            vr = vt[0, :, cols]
            vi = vt[1, :, cols]
            for kb in range(16):
                tiles = [[], [], []]
                for c in (0, 2):
                    q = kb * 4 + c
                    ur = jnp.where(first, ut[0, q : q + 1, cols], ut[0, q + 1 : q + 2, cols])
                    ui = jnp.where(first, ut[1, q : q + 1, cols], ut[1, q + 1 : q + 2, cols])
                    re = ur * vr - ui * vi
                    im = -(ui * vr + ur * vi)
                    for tile, value in zip(tiles, (re, re + im, im - re)):
                        tile.append(value)
                for p in range(3):
                    hi, lo = split(jnp.concatenate(tiles[p], 0))
                    th[h, p, kb, :, cols] = hi
                    tl[h, p, kb, :, cols] = lo

    def split_x(t):
        @pl.loop(0, 8)
        def _(b):
            rows = pl.ds(pl.multiple_of(b * 128, 128), 128)
            re = xf[t, 0, rows, :]
            im = xf[t, 1, rows, :]
            for p, value in enumerate((re + im, im, re)):
                hi, lo = split(value)
                xh[t, p, rows, :] = hi
                xl[t, p, rows, :] = lo

    def gen_cols():
        for b in range(4):
            jj = b * 256 + iota((1, 256), 1)
            cos, sin = cos_sin((col_of[...] * (coff[0] + jj)) & MASK)
            w = window(jj)
            ph[0, :, b * 256 : (b + 1) * 256] = w * cos
            ph[1, :, b * 256 : (b + 1) * 256] = -(w * sin)

        lane = iota((1, M), 1)
        cos, sin = cos_sin((lane * (coff[0] + 8 * iota((F // 8, 1), 0))) & MASK)
        wt[0] = cos
        wt[1] = sin
        c1, s1 = cos_sin((lane * iota((8, 1), 0)) & MASK)

        @pl.loop(0, 16)
        def _(b):
            eight = pl.ds(pl.multiple_of(b * 8, 8), 8)
            wc = wt[0, eight, :]
            ws = wt[1, eight, :]
            for k in range(0, 8, 2):
                pair = []
                for n in (k, k + 1):
                    c0 = wc[n : n + 1]
                    s0 = ws[n : n + 1]
                    pair.append(jnp.concatenate([c0 * c1 - s0 * s1, -(s0 * c1 + c0 * s1)], 1))
                hi, lo = split(jnp.concatenate(pair, 0))
                rows = pl.ds(pl.multiple_of(b * 64 + k * 8, 16), 16)
                eh[rows, :] = hi
                el[rows, :] = lo

    def matmul(u, half):
        h, t = divmod(u, NT)
        rows = pl.ds(8 * half, 8)
        k1, k2, k3 = (
            dot3(
                th[h, p, rows].reshape(128, F), tl[h, p, rows].reshape(128, F), xh[t, p], xl[t, p]
            )
            for p in range(3)
        )
        re = (k1 - k2).reshape(2, 2, 2, 2, 8, CW)
        im = (k1 + k3).reshape(2, 2, 2, 2, 8, CW)
        for pair in range(2):
            s[u, half, :, :, :, 2 * pair] = re[:, :, :, pair]
            s[u, half, :, :, :, 2 * pair + 1] = im[:, :, :, pair]

    def d2d(u):
        return pltpu.make_async_remote_copy(
            src_ref=s.at[u, 1 - core],
            dst_ref=rd.at[u],
            send_sem=d_ssem.at[u],
            recv_sem=d_rsem.at[u],
            device_id=(i ^ 1, j),
            device_id_type=MESH,
        )

    def region(order, k, c0, n, other):
        sel = [slice(None)] * 3
        for d in order[:k]:
            sel[d] = own[d]
        sel[order[k]] = 1 - own[order[k]] if other else own[order[k]]
        return (*sel, slice(c0, c0 + n))

    def exchange(u, k, gi):
        order, c0, n = groups_of(u)[gi]
        return pltpu.make_async_remote_copy(
            src_ref=s.at[(u, core, *region(order, k, c0, n, True))],
            dst_ref=recv_bufs[k].at[(u, *[slice(None)] * (2 - k), slice(c0, c0 + n))],
            send_sem=e_ssem.at[u, k, gi],
            recv_sem=e_rsem.at[u, k, gi],
            device_id=(i ^ FLIP[order[k]], j),
            device_id_type=MESH,
        )

    def finish_d2d(u):
        d2d(u).wait_recv()
        s[u, core] += rd[u]
        if u >= STEPPED:
            for d in PIECES:
                direct(u, d).start()
        else:
            for gi in range(3):
                exchange(u, 0, gi).start()

    def direct(u, d):
        to = (own[0] ^ (d >> 2), own[1] ^ ((d >> 1) & 1), own[2] ^ (d & 1))
        return pltpu.make_async_remote_copy(
            src_ref=s.at[(u, core, *to)],
            dst_ref=r7.at[u - STEPPED, d],
            send_sem=f_ssem.at[u - STEPPED, d],
            recv_sem=f_rsem.at[u - STEPPED, d],
            device_id=(i ^ flip_of(d), j),
            device_id_type=MESH,
        )

    def finish_direct(u):
        total = s[(u, core, *own)]
        for d in PIECES:
            direct(u, d).wait_recv()
            total = total + r7[u - STEPPED, d]
        s[(u, core, *own)] = total

    def finish_exchange(u, k):
        for gi, (order, c0, n) in enumerate(groups_of(u)):
            exchange(u, k, gi).wait_recv()
            at = (u, core, *region(order, k, c0, n, False))
            s[at] += recv_bufs[k][(u, *[slice(None)] * (2 - k), slice(c0, c0 + n))]
            if k < 2:
                exchange(u, k + 1, gi).start()

    sign = jnp.where(iota((8, 1), 0) < 4, -1.0, 1.0).astype(f32)

    def columns(u):
        h, t = divmod(u, NT)
        cols = slice(t * CW, (t + 1) * CW)
        for pair in range(2):
            re = s[u, core, own[0], own[1], own[2], 2 * pair]
            im = s[u, core, own[0], own[1], own[2], 2 * pair + 1]
            fb[0, 2 * pair] = jnp.concatenate([re[:4], im[:4]], 0)
            fb[1, 2 * pair] = jnp.concatenate([-im[:4], re[:4]], 0)
            fb[0, 2 * pair + 1] = jnp.concatenate([re[4:], im[4:]], 0)
            fb[1, 2 * pair + 1] = jnp.concatenate([-im[4:], re[4:]], 0)
        for q0 in range(0, SLOTS, 4):
            tiles = []
            for q in range(q0, q0 + 4):
                st = strip_of[0, q]
                tiles.append(fb[0, st] * ph[0, q : q + 1, cols] + fb[1, st] * ph[1, q : q + 1, cols])
            hi, lo = split(jnp.concatenate(tiles, 0))
            ah[q0 * 8 : (q0 + 4) * 8, :] = hi
            al[q0 * 8 : (q0 + 4) * 8, :] = lo
        prod = dot3(ah[...], al[...], eh[cols, :], el[cols, :])
        if t == 0:
            gacc[h] = prod
        elif t < NT - 1:
            gacc[h] += prod
        else:
            total = (gacc[h] + prod).reshape(SLOTS, 8, 2 * M)
            cross = total[:, :, M:]
            cross = jnp.concatenate([cross[:, 4:], cross[:, :4]], 1)
            g[h] = total[:, :, :M] + cross * sign

    def a_copy(h, a):
        return pltpu.make_async_remote_copy(
            src_ref=g.at[h, pl.ds(3 * a, 3)],
            dst_ref=ra.at[h, xhi, kz],
            send_sem=a_ssem.at[h, a],
            recv_sem=a_rsem.at[h, xhi, kz],
            device_id=(a, z * 2 + core),
            device_id_type=MESH,
        )

    def start_a(h):
        for d in range(15, 0, -1):
            a_copy(h, i ^ d).start()

        @pl.when(core != xhi)
        def _():
            a_copy(h, i).start()

        @pl.when(core == xhi)
        def _():
            ra[h, xhi, kz] = g[h, pl.ds(3 * i, 3)]

    def end_a(h):
        for d in range(15, 0, -1):
            a_copy(h, i ^ d).wait_send()

        @pl.when(core != xhi)
        def _():
            a_copy(h, i).wait_send()

    def b_copy(h, k):
        return pltpu.make_async_remote_copy(
            src_ref=pb.at[h, k],
            dst_ref=rb.at[h, z],
            send_sem=b_ssem.at[h, k],
            recv_sem=b_rsem.at[h, z],
            device_id=(i, k * 2 + xhi),
            device_id_type=MESH,
        )

    def a_arrival(h, xs, k):
        return pltpu.make_async_remote_copy(
            src_ref=g.at[h, pl.ds(0, 3)],
            dst_ref=ra.at[h, xs, k],
            send_sem=a_ssem.at[h, 0],
            recv_sem=a_rsem.at[h, xs, k],
            device_id=(i, j),
            device_id_type=MESH,
        )

    def b_arrival(h, zs):
        return pltpu.make_async_remote_copy(
            src_ref=pb.at[h, 0],
            dst_ref=rb.at[h, zs],
            send_sem=b_ssem.at[h, 0],
            recv_sem=b_rsem.at[h, zs],
            device_id=(i, j),
            device_id_type=MESH,
        )

    def finish_a(h):
        for d in (1, 2, 3, 4, 5, 6, 7, 0):
            k = z ^ d
            a_arrival(h, 1 - xhi, k).wait_recv()

            @pl.when(jnp.logical_or(core != xhi, k != kz))
            def _():
                a_arrival(h, xhi, k).wait_recv()

            pb[h, k] = ra[h, 0, k] + ra[h, 1, k]
            if d:
                b_copy(h, k).start()

    def finish_b(h):
        total = pb[h, z]
        for d in range(1, 8):
            b_arrival(h, z ^ d).wait_recv()
            total = total + rb[h, z ^ d]
        out_ref[:, 0, 4 * h : 4 * h + 4, :] = total[:, :4]
        out_ref[:, 1, 4 * h : 4 * h + 4, :] = total[:, 4:]

    def end_b(h):
        for d in range(1, 8):
            b_copy(h, z ^ d).wait_send()

    def end_strips():
        for u in range(2 * NT):
            d2d(u).wait_send()
            for d in PIECES if u >= STEPPED else ():
                direct(u, d).wait_send()
            for k in range(3 if u < STEPPED else 0):
                for gi in range(3):
                    exchange(u, k, gi).wait_send()

    def product(u):
        if u < NT:
            x_copy(u).wait()
            split_x(u)
        if u < LAST:
            matmul(u, 0)
            matmul(u, 1)
            if u == 0:
                wait_barrier()
            d2d(u).start()
        else:
            matmul(u, 1 - core)
            d2d(u).start()
            matmul(u, core)

    for copy in scalar_copies():
        copy.wait()
    gen_slots()
    strip_copy().start()
    gen_u()
    gen_v(0)
    gen_t(0)
    for kind, *at in PLAN:
        if kind == "m":
            product(*at)
        elif kind == "d":
            finish_d2d(*at)
        elif kind == "e":
            finish_exchange(*at)
        elif kind == "f":
            finish_direct(*at)
        elif kind == "t":
            gen_v(1)
            gen_t(1)
        elif kind == "g":
            strip_copy().wait()
            gen_cols()
        elif kind == "c":
            columns(*at)
        elif kind == "s":
            start_a(*at)
        elif kind == "w":
            end_strips()
        elif kind == "a":
            finish_a(*at)
        elif kind == "x":
            end_a(*at)
        elif kind == "b":
            finish_b(*at)
        elif kind == "y":
            end_b(*at)


PLAN = (
    ("m", 0),
    ("m", 1), ("d", 0),
    ("m", 2), ("d", 1),
    ("m", 3), ("d", 2), ("e", 0, 0),
    ("t",), ("d", 3),
    ("m", 4), ("e", 1, 0),
    ("m", 5), ("e", 2, 0), ("e", 0, 1), ("d", 4),
    ("m", 6), ("e", 1, 1), ("d", 5),
    ("m", 7), ("e", 2, 1), ("d", 6), ("d", 7),
    ("g",), ("e", 0, 2), ("c", 0), ("f", 4), ("c", 4), ("e", 1, 2), ("c", 1), ("e", 2, 2), ("c", 2), ("f", 3), ("c", 3), ("s", 0),
    ("f", 5), ("c", 5), ("f", 6), ("c", 6), ("w",), ("f", 7), ("c", 7), ("s", 1),
    ("a", 0), ("x", 0), ("a", 1), ("x", 1), ("b", 0), ("y", 0), ("b", 1), ("y", 1),
)


def per_device(facets, row_off, col_off, strip_offset, subgrid_strip, subgrid_column, subgrid_slot):
    vmem = pl.BlockSpec(memory_space=pltpu.VMEM)
    dma = pltpu.SemaphoreType.DMA
    u = 2 * NT
    return pl.pallas_call(
        kernel,
        out_shape=jax.ShapeDtypeStruct((3, 2, 8, M), f32),
        in_specs=[pl.BlockSpec(memory_space=pl.ANY)] * 7,
        out_specs=vmem,
        scratch_shapes=[
            *(pltpu.SMEM((n,), jnp.int32) for n in (1, 1, 4, SLOTS, SLOTS, SLOTS)),
            pltpu.VMEM((1, 128), jnp.int32),
            pltpu.SMEM((1, 128), jnp.int32),
            pltpu.VMEM((SLOTS, 1), jnp.int32),
            pltpu.VMEM((NT, 2, F, CW), f32),
            pltpu.VMEM((NT, 3, F, CW), bf16),
            pltpu.VMEM((NT, 3, F, CW), bf16),
            pltpu.VMEM((2, 3, 16, 16, F), bf16),
            pltpu.VMEM((2, 3, 16, 16, F), bf16),
            pltpu.VMEM((2, 64, F), f32),
            pltpu.VMEM((2, 8, F), f32),
            pltpu.VMEM((2, F // 8, M), f32),
            pltpu.VMEM((u, 2, 2, 2, 2, 4, 8, CW), f32),
            pltpu.VMEM((u, 2, 2, 2, 4, 8, CW), f32),
            pltpu.VMEM((STEPPED, 2, 2, 4, 8, CW), f32),
            pltpu.VMEM((STEPPED, 2, 4, 8, CW), f32),
            pltpu.VMEM((STEPPED, 4, 8, CW), f32),
            pltpu.VMEM((u - STEPPED, 8, 4, 8, CW), f32),
            pltpu.VMEM((2, 4, 8, CW), f32),
            pltpu.VMEM((2, SLOTS, F), f32),
            pltpu.VMEM((F, 2 * M), bf16),
            pltpu.VMEM((F, 2 * M), bf16),
            pltpu.VMEM((SLOTS * 8, CW), bf16),
            pltpu.VMEM((SLOTS * 8, CW), bf16),
            pltpu.VMEM((2, SLOTS * 8, 2 * M), f32),
            pltpu.VMEM((2, SLOTS, 8, M), f32),
            pltpu.VMEM((2, 2, 8, 3, 8, M), f32),
            pltpu.VMEM((2, 8, 3, 8, M), f32),
            pltpu.VMEM((2, 8, 3, 8, M), f32),
            dma((NT,)),
            dma((1,)),
            dma((6,)),
            dma((u,)),
            dma((u,)),
            dma((STEPPED, 3, 3)),
            dma((STEPPED, 3, 3)),
            dma((u - STEPPED, 8)),
            dma((u - STEPPED, 8)),
            dma((2, 16)),
            dma((2, 2, 8)),
            dma((2, 8)),
            dma((2, 8)),
        ],
        compiler_params=pltpu.CompilerParams(
            collective_id=0, has_side_effects=True, vmem_limit_bytes=56 * 1024 * 1024
        ),
        name="facet_to_subgrid",
    )(facets, row_off, col_off, strip_offset, subgrid_strip, subgrid_column, subgrid_slot)


def solution(mesh):
    placed = (P(None, "frow", "fcol"), P("frow"), P("fcol"), P(), P(), P(), P())
    return jax.shard_map(
        per_device,
        mesh=mesh,
        in_specs=placed,
        out_specs=P("frow", None, "fcol", None),
        check_vma=False,
    )
```
